512 devices in a mesh: mem: 128 (over x, z, core), grp: 4 (over y).
Axes of the slice: x: 4, y: 4, z: 16, core: 2. Of those that a mesh axis runs over, the one named last changes fastest.
Arguments:
- prior_members: bfloat16 [256, 512, 256], P('mem', 'grp'), may hold values from -6 to 6
- mapped_prior: bfloat16 [256, 512, 1024], P('mem', 'grp'), may hold values from -6 to 6
- departure: float32 [512, 1024], P(('grp', 'mem')), may hold values from -18 to 18
- precision_factor: float32 [512, 1024], P(('grp', 'mem')), may hold values from 0.02 to 0.5
- measured_lines: int32 [512], P(('grp', 'mem')), may hold values from 256 to 1024, as said below
Outputs:
- analysis: bfloat16 [256, 512, 256], P('mem', 'grp')
The draws below stay inside these ranges and needn't reach their ends.
Inputs may be any that keep to these rules, and one draw needn't show every extreme that they name: Only the first measured_lines rows of a patch's observation block are used; some patch has exactly 1024 rows and some exactly 256.
All inputs are finite; a program needn't handle non-finite values.
Results may differ from the reference program's by a relative error of at most 0.008.
Values may be sent and summed in bfloat16 or wider, within the bound.
A program may use at most 64 MiB of HBM per device.

```python
import math
import jax
import jax.numpy as jnp
from jax import lax

MEMBER_NUMBER = 256
DOMAIN_UNKNOWNS = 256
OBS_MAX = 1024
ITERS = 5
DOMAIN_NUMBER = 512


def draw_measured_lines(key, part):
    lowest = OBS_MAX // 4
    spread = OBS_MAX - lowest
    key_rows = jax.random.fold_in(key, 11)
    key_high = jax.random.fold_in(key, 12)
    key_low = jax.random.fold_in(key, 13)
    draws = jax.random.randint(key_rows, (DOMAIN_NUMBER,), 0, spread + 1, dtype=jnp.int32)
    squared = draws * draws // spread
    counts = lowest + squared * draws // spread
    high_pos = jax.random.randint(key_high, (), 0, DOMAIN_NUMBER, dtype=jnp.int32)
    low_pos = (high_pos + 1 + jax.random.randint(key_low, (), 0, DOMAIN_NUMBER - 1, dtype=jnp.int32)) % DOMAIN_NUMBER
    positions = jnp.arange(DOMAIN_NUMBER, dtype=jnp.int32)
    counts = jnp.where(positions == high_pos, OBS_MAX, counts)
    counts = jnp.where(positions == low_pos, lowest, counts)
    return counts.astype(jnp.int32)


def block_scale(rng, extent, split, smallest, top_value):
    factor_of, own = 1.0, jax.random.fold_in(rng, 6)
    for dim, parts in split:
        steps = jnp.exp(jax.random.uniform(jax.random.fold_in(own, dim), (parts,), jnp.float32, smallest / len(split), top_value / len(split)))
        factor_of = factor_of * jnp.repeat(steps, extent[dim] // parts).reshape([-1 if axis == dim else 1 for axis in range(len(extent))])
    return factor_of


def normal_values(stream_key, dims, width, bound, shards=(), kind=jnp.bfloat16):
    drawn = jax.random.normal(stream_key, dims, jnp.float32) * width
    if len(shards) > 0:
        drawn = block_scale(stream_key, dims, shards, -0.22, 0.18) * drawn
    return jnp.clip(drawn, min=-bound, max=bound).astype(kind)


def setup_inputs(seed: int = 0) -> dict:
    seeds = jax.random.split(jax.random.key(seed), 6)
    prior_members = normal_values(seeds[0], (MEMBER_NUMBER, DOMAIN_NUMBER, DOMAIN_UNKNOWNS), 1.0, 6.0, ((0, 128), (1, 4)))
    mapped_prior = normal_values(seeds[1], (MEMBER_NUMBER, DOMAIN_NUMBER, OBS_MAX), 1.0, 6.0, ((0, 128), (1, 4)))
    departure = normal_values(seeds[2], (DOMAIN_NUMBER, OBS_MAX), 3.0, 18.0, ((0, 512),), jnp.float32)
    precision_factor = jnp.clip(jnp.exp(math.log(0.5) - 3.218876 * jax.random.uniform(seeds[3], (DOMAIN_NUMBER, OBS_MAX), jnp.float32) ** block_scale(seeds[3], (DOMAIN_NUMBER, OBS_MAX), ((0, 512),), -0.2, 0.2)), 0.02, 0.5)
    measured_lines = draw_measured_lines(jax.random.fold_in(seeds[5], 71), 0)
    return dict(prior_members=prior_members, mapped_prior=mapped_prior, departure=departure, precision_factor=precision_factor, measured_lines=measured_lines)


highest = lax.Precision.HIGHEST

def local_posterior(prior_local_members, measurement_data, departure_line, line_precision_list, lines_in_play):
    grid_quantities = prior_local_members.astype(jnp.float32)
    center = lax.optimization_barrier(jnp.mean(grid_quantities, axis=0))
    spread = grid_quantities - center[None, :]
    values = measurement_data.astype(jnp.float32)
    deviat = values - lax.optimization_barrier(jnp.mean(values, axis=0, keepdims=True))
    row_ids = jnp.arange(OBS_MAX, dtype=jnp.int32)
    weights = jnp.where(row_ids < lines_in_play, line_precision_list, jnp.float32(0.0))
    weighted = deviat * weights[None, :]
    gram_total = jnp.dot(weighted, deviat.T, precision=highest)
    pull_vec = jnp.dot(weighted, departure_line, precision=highest)
    identity = jnp.eye(MEMBER_NUMBER, dtype=jnp.float32)
    system = gram_total + jnp.float32(MEMBER_NUMBER - 1) * identity
    fro_scale = jnp.sqrt(jnp.sum(system * system))
    iterate = system / fro_scale
    inv_root = identity
    for sweep in range(ITERS):
        factor = 0.5 * (3.0 * identity - jnp.dot(inv_root, iterate, precision=highest))
        iterate = jnp.dot(iterate, factor, precision=highest)
        inv_root = jnp.dot(factor, inv_root, precision=highest)
    inner = jnp.dot(inv_root, pull_vec, precision=highest)
    mean_shift = jnp.dot(inv_root, inner, precision=highest) / fro_scale
    transform = math.sqrt(MEMBER_NUMBER - 1) / jnp.sqrt(fro_scale) * inv_root + mean_shift[:, None]
    result = center[None, :] + jnp.dot(transform.T, spread, precision=highest)
    return result.astype(jnp.bfloat16)

def reference(prior_members, mapped_prior, departure, precision_factor, measured_lines):

    def patch_case(domain_number):
        return local_posterior(prior_members[:, domain_number], mapped_prior[:, domain_number], departure[domain_number], precision_factor[domain_number], measured_lines[domain_number])
    result = lax.map(patch_case, jnp.arange(DOMAIN_NUMBER, dtype=jnp.int32))
    return jnp.transpose(result, (1, 0, 2))
```

```python
import functools
import math

import jax
import jax.numpy as jnp
from jax import lax
from jax.experimental import pallas as pl
from jax.experimental.pallas import tpu as pltpu
from jax.sharding import Mesh
from jax.sharding import PartitionSpec as P

ITERS = 5
OWN = 2
CHUNK = 256
MEM = ("x", "z", "c")
GRP_MEM = ("grp", "x", "z", "c")
MESH_ID = pl.DeviceIdType.MESH

highest = lax.Precision.HIGHEST
f32 = jnp.float32
bf16 = jnp.bfloat16


def one_hot(rows, source_of):
    out_row = lax.broadcasted_iota(jnp.int32, (rows, rows), 0)
    in_row = lax.broadcasted_iota(jnp.int32, (rows, rows), 1)
    return jnp.where(in_row == source_of(out_row), f32(1.0), f32(0.0)).astype(bf16)


def moved(perm, rows):
    return jnp.dot(perm, rows, preferred_element_type=f32).astype(bf16)


def kernel(
    nx, nz, nc,
    prior_hbm, mapped_hbm, dep_ref, prec_ref, lines_ref, out_ref,
    raw, split_a, split_z, back_z, back_a, s1, ar, s2, zr, s3, zb, s4, ab, gram, pull, root, itr,
    raw_sem, a_send, a_recv, z_send, z_recv, zb_send, zb_recv, ab_send, ab_recv,
):
    na = nx * nc
    members = OWN * na * nz
    obs_chunks = mapped_hbm.shape[2] // CHUNK
    chunks = obs_chunks + 1
    patches = nx * nz * nc
    x, z, c = lax.axis_index("x"), lax.axis_index("z"), lax.axis_index("c")
    a = x * nc + c

    def raw_copies(k):
        if k < obs_chunks:
            src = lambda m: mapped_hbm.at[m, :, pl.ds(k * CHUNK, CHUNK)]
        else:
            src = lambda m: prior_hbm.at[m]
        return [
            pltpu.make_async_copy(src(m), raw.at[k, pl.ds(m * patches, patches)], raw_sem.at[k, m])
            for m in range(OWN)
        ]

    for k in range(chunks):
        for copy in raw_copies(k):
            copy.start()

    barrier = pltpu.get_barrier_semaphore()

    def greet_z(j, _):
        pl.semaphore_signal(
            barrier, inc=1, device_id={"z": lax.rem(z + j, nz)}, device_id_type=MESH_ID
        )
        return 0

    def greet_a(j, _):
        t = lax.rem(a + j, na)
        pl.semaphore_signal(
            barrier, inc=1, device_id={"x": t // nc, "c": lax.rem(t, nc)}, device_id_type=MESH_ID
        )
        return 0

    lax.fori_loop(1, nz, greet_z, 0)
    lax.fori_loop(1, na, greet_a, 0)

    split_a[...] = one_hot(
        members,
        lambda r: (r % OWN) * patches
        + (r // (OWN * nz * nc)) * (nz * nc)
        + ((r // OWN) % nz) * nc
        + (r // (OWN * nz)) % nc,
    )
    split_z[...] = one_hot(
        members, lambda r: ((r // OWN) % na) * (OWN * nz) + (r // (OWN * na)) * OWN + r % OWN
    )
    back_z[...] = one_hot(
        members, lambda r: ((r // OWN) % nz) * (OWN * na) + (r // (OWN * nz)) * OWN + r % OWN
    )
    back_a[...] = one_hot(
        members,
        lambda r: ((r // (nz * nc)) % nx) * (OWN * nz * nc)
        + (r % nc) * (OWN * nz)
        + ((r // nc) % nz) * OWN
        + r // patches,
    )

    def a_copy(src, dst, send, recv, j):
        t = lax.rem(a + j, na)
        return pltpu.make_async_remote_copy(
            src_ref=src.at[t], dst_ref=dst.at[a], send_sem=send, recv_sem=recv,
            device_id={"x": t // nc, "c": lax.rem(t, nc)}, device_id_type=MESH_ID,
        )

    def z_copy(src, dst, send, recv, j):
        step = ((j + 1) // 2) * (1 - 2 * (j % 2))
        t = lax.rem(z + nz // 2 + step, nz)
        return pltpu.make_async_remote_copy(
            src_ref=src.at[t], dst_ref=dst.at[z], send_sem=send, recv_sem=recv,
            device_id={"z": t}, device_id_type=MESH_ID,
        )

    def all_a(src, dst, send, recv):
        def body(j, _):
            a_copy(src, dst, send, recv, j).start()
            return 0

        lax.fori_loop(1, na, body, 0)

    def all_z(src, dst, send, recv):
        def body(j, _):
            z_copy(src, dst, send, recv, j).start()
            return 0

        lax.fori_loop(0, nz - 1, body, 0)

    def arrived(ref, sem, n):
        part = ref.at[pl.ds(0, n)]
        pltpu.make_async_copy(part, part, sem).wait()

    def stage_one(k):
        for copy in raw_copies(k):
            copy.wait()
        s1[k] = moved(split_a[...], raw[k]).reshape(s1.shape[1:])
        ar[k, a] = s1[k, a]

    stage_one(0)
    pl.semaphore_wait(barrier, (nz - 1) + (na - 1))
    all_a(s1.at[0], ar.at[0], a_send.at[0], a_recv.at[0])
    for k in range(1, chunks):
        stage_one(k)
        all_a(s1.at[k], ar.at[k], a_send.at[k], a_recv.at[k])

    for k in range(chunks):
        arrived(ar.at[k], a_recv.at[k], na - 1)
        s2[k] = moved(split_z[...], ar[k].reshape(members, CHUNK)).reshape(s2.shape[1:])
        all_z(s2.at[k], zr.at[k], z_send.at[k], z_recv.at[k])
        zr[k, z] = s2[k, z]

    lines = lines_ref[0]
    eye = (
        lax.broadcasted_iota(jnp.int32, (members, members), 0)
        == lax.broadcasted_iota(jnp.int32, (members, members), 1)
    )
    identity = jnp.where(eye, f32(1.0), f32(0.0))
    gram[...] = f32(members - 1) * identity
    pull[...] = jnp.zeros_like(pull)
    for k in range(obs_chunks):
        arrived(zr.at[k], z_recv.at[k], nz - 1)
        values = zr[k].reshape(members, CHUNK).astype(f32)
        deviat = values - jnp.mean(values, axis=0, keepdims=True)
        row_ids = k * CHUNK + lax.broadcasted_iota(jnp.int32, (1, CHUNK), 1)
        cols = pl.ds(k * CHUNK, CHUNK)
        weights = jnp.where(row_ids < lines, prec_ref[:, cols], f32(0.0))
        weighted = deviat * weights
        gram[...] += lax.dot_general(
            weighted, deviat, (((1,), (1,)), ((), ())), precision=highest,
            preferred_element_type=f32,
        )
        pull[...] += jnp.sum(weighted * dep_ref[:, cols], axis=1, keepdims=True)

    def dot(p, q):
        return jnp.dot(p, q, precision=highest, preferred_element_type=f32)

    system = gram[...]
    scale = jnp.sqrt(jnp.sum(jnp.sum(system * system, axis=1, keepdims=True), axis=0, keepdims=True))
    itr[...] = system / scale
    root[...] = identity
    for sweep in range(ITERS):
        if sweep == 0:
            factor = 1.5 * identity - 0.5 * itr[...]
            root[...] = factor
        else:
            factor = 1.5 * identity - 0.5 * dot(root[...], itr[...])
            root[...] = dot(factor, root[...])
        if sweep < ITERS - 1:
            itr[...] = dot(itr[...], factor)

    inv_root = root[...]
    inner = jnp.sum(inv_root * pull[...], axis=0, keepdims=True)
    shift = jnp.sum(inv_root * inner, axis=1, keepdims=True) / scale
    shift = jnp.sum(jnp.where(eye, shift, f32(0.0)), axis=0, keepdims=True)
    transform = (math.sqrt(members - 1) / jnp.sqrt(scale)) * inv_root + shift

    arrived(zr.at[obs_chunks], z_recv.at[obs_chunks], nz - 1)
    quantities = zr[obs_chunks].reshape(members, CHUNK).astype(f32)
    center = jnp.mean(quantities, axis=0, keepdims=True)
    result = center + dot(transform, quantities - center)
    s3[...] = result.astype(bf16).reshape(s3.shape)
    all_z(s3, zb, zb_send, zb_recv)
    zb[z] = s3[z]
    arrived(zb, zb_recv, nz - 1)
    s4[...] = moved(back_z[...], zb[...].reshape(members, CHUNK)).reshape(s4.shape)
    all_a(s4, ab, ab_send, ab_recv)
    ab[a] = s4[a]
    arrived(ab, ab_recv, na - 1)
    out_ref[...] = moved(back_a[...], ab[...].reshape(members, CHUNK)).reshape(out_ref.shape)

    for k in range(chunks):
        arrived(s1.at[k], a_send.at[k], na - 1)
        arrived(s2.at[k], z_send.at[k], nz - 1)
    arrived(s3, zb_send, nz - 1)
    arrived(s4, ab_send, na - 1)


def solution(mesh):
    nx, nz, nc = 4, 16, 2
    split = Mesh(mesh.devices.reshape(nx, nz, nc, mesh.shape["grp"]), ("x", "z", "c", "grp"))
    na = nx * nc
    members = OWN * na * nz

    def local(prior_members, mapped_prior, departure, precision_factor, measured_lines):
        chunks = mapped_prior.shape[2] // CHUNK + 1
        square = pltpu.VMEM((members, members), f32)
        perm = pltpu.VMEM((members, members), bf16)
        by_a = (na, OWN * nz, CHUNK)
        by_z = (nz, OWN * na, CHUNK)
        dma = pltpu.SemaphoreType.DMA
        return pl.pallas_call(
            functools.partial(kernel, nx, nz, nc),
            out_shape=jax.ShapeDtypeStruct(prior_members.shape, bf16),
            in_specs=[
                pl.BlockSpec(memory_space=pl.ANY),
                pl.BlockSpec(memory_space=pl.ANY),
                pl.BlockSpec(memory_space=pltpu.VMEM),
                pl.BlockSpec(memory_space=pltpu.VMEM),
                pl.BlockSpec(memory_space=pltpu.SMEM),
            ],
            out_specs=pl.BlockSpec(memory_space=pltpu.VMEM),
            scratch_shapes=[
                pltpu.VMEM((chunks, members, CHUNK), bf16),
                perm, perm, perm, perm,
                pltpu.VMEM((chunks, *by_a), bf16),
                pltpu.VMEM((chunks, *by_a), bf16),
                pltpu.VMEM((chunks, *by_z), bf16),
                pltpu.VMEM((chunks, *by_z), bf16),
                pltpu.VMEM(by_z, bf16),
                pltpu.VMEM(by_z, bf16),
                pltpu.VMEM(by_a, bf16),
                pltpu.VMEM(by_a, bf16),
                square,
                pltpu.VMEM((members, 1), f32),
                square,
                square,
                dma((chunks, OWN)),
                dma((chunks,)), dma((chunks,)),
                dma((chunks,)), dma((chunks,)),
                dma, dma, dma, dma,
            ],
            compiler_params=pltpu.CompilerParams(
                collective_id=0, has_side_effects=True, vmem_limit_bytes=48 << 20
            ),
        )(prior_members, mapped_prior, departure, precision_factor, measured_lines)

    return jax.shard_map(
        local,
        mesh=split,
        in_specs=(
            P(MEM, "grp", None),
            P(MEM, "grp", None),
            P(GRP_MEM, None),
            P(GRP_MEM, None),
            P(GRP_MEM),
        ),
        out_specs=P(MEM, "grp", None),
        check_vma=False,
    )
```

```python
import functools
import math

import jax
import jax.numpy as jnp
from jax import lax
from jax.experimental import pallas as pl
from jax.experimental.pallas import tpu as pltpu
from jax.sharding import Mesh
from jax.sharding import PartitionSpec as P

ITERS = 5
OWN = 2
CHUNK = 256
HALF = CHUNK // 2
MEM = ("x", "z", "c")
GRP_MEM = ("grp", "x", "z", "c")
MESH_ID = pl.DeviceIdType.MESH

highest = lax.Precision.HIGHEST
f32 = jnp.float32
bf16 = jnp.bfloat16


def one_hot(rows, source_of):
    out_row = lax.broadcasted_iota(jnp.int32, (rows, rows), 0)
    in_row = lax.broadcasted_iota(jnp.int32, (rows, rows), 1)
    return jnp.where(in_row == source_of(out_row), f32(1.0), f32(0.0)).astype(bf16)


def moved(perm, rows):
    return jnp.dot(perm, rows, preferred_element_type=f32).astype(bf16)


def kernel(
    nx, nz, nc,
    prior_hbm, mapped_hbm, dep_hbm, prec_hbm, lines_ref, out_ref,
    raw, dep_ref, prec_ref, split_a, split_z, back_z, back_a, nat_z, z_nat, s1, ar, s2, zr, s3, zb, s4, ab, gram, pull, root, itr,
    raw_sem, row_sem, a_send, a_recv, z_send, z_recv, zb_send, zb_recv, ab_send, ab_recv,
):
    na = nx * nc
    members = OWN * na * nz
    obs_chunks = mapped_hbm.shape[2] // CHUNK
    chunks = obs_chunks + 1
    patches = nx * nz * nc
    x, z, c = lax.axis_index("x"), lax.axis_index("z"), lax.axis_index("c")
    a = x * nc + c

    def raw_copies(k):
        if k < obs_chunks:
            src = lambda m: mapped_hbm.at[m, :, pl.ds(k * CHUNK, CHUNK)]
        else:
            src = lambda m: prior_hbm.at[m]
        return [
            pltpu.make_async_copy(src(m), raw.at[k, pl.ds(m * patches, patches)], raw_sem.at[k, m])
            for m in range(OWN)
        ]

    row_copies = [
        pltpu.make_async_copy(dep_hbm, dep_ref, row_sem.at[0]),
        pltpu.make_async_copy(prec_hbm, prec_ref, row_sem.at[1]),
    ]
    for k in range(chunks):
        for copy in raw_copies(k):
            copy.start()
    for copy in row_copies:
        copy.start()

    barrier = pltpu.get_barrier_semaphore()

    def greet_z(j, _):
        pl.semaphore_signal(
            barrier, inc=1, device_id={"z": lax.rem(z + j, nz)}, device_id_type=MESH_ID
        )
        return 0

    def greet_a(j, _):
        t = lax.rem(a + j, na)
        pl.semaphore_signal(
            barrier, inc=1, device_id={"x": t // nc, "c": lax.rem(t, nc)}, device_id_type=MESH_ID
        )
        return 0

    lax.fori_loop(1, nz, greet_z, 0)
    lax.fori_loop(1, na, greet_a, 0)

    def natural(m, xi, zi, ci):
        return m * patches + xi * (nz * nc) + zi * nc + ci

    def of_natural(r):
        return r // patches, (r // (nz * nc)) % nx, (r // nc) % nz, r % nc

    def of_group(r):
        return r % OWN, r // (OWN * nz * nc), (r // OWN) % nz, (r // (OWN * nz)) % nc

    def of_ring(r):
        return r % OWN, (r // (OWN * nc)) % nx, r // (OWN * na), (r // OWN) % nc

    def group(m, xi, zi, ci):
        return ((xi * nc + ci) * nz + zi) * OWN + m

    def ring(m, xi, zi, ci):
        return ((zi * nx + xi) * nc + ci) * OWN + m

    nat_z[...] = one_hot(members, lambda r: natural(*of_ring(r)))
    split_a[...] = one_hot(members, lambda r: natural(*of_group(r)))
    split_z[...] = one_hot(members, lambda r: group(*of_ring(r)))
    back_z[...] = one_hot(members, lambda r: ring(*of_group(r)))
    back_a[...] = one_hot(members, lambda r: group(*of_natural(r)))
    z_nat[...] = one_hot(members, lambda r: ring(*of_natural(r)))

    def a_copy(src, dst, send, recv, j):
        t = lax.rem(a + j, na)
        return pltpu.make_async_remote_copy(
            src_ref=src.at[t], dst_ref=dst.at[a], send_sem=send, recv_sem=recv,
            device_id={"x": t // nc, "c": lax.rem(t, nc)}, device_id_type=MESH_ID,
        )

    def z_copy(src, dst, send, recv, j):
        step = ((j + 1) // 2) * (1 - 2 * (j % 2))
        t = lax.rem(z + nz // 2 + step, nz)
        return pltpu.make_async_remote_copy(
            src_ref=src.at[t], dst_ref=dst.at[z], send_sem=send, recv_sem=recv,
            device_id={"z": t}, device_id_type=MESH_ID,
        )

    def all_a(src, dst, send, recv):
        def body(j, _):
            a_copy(src, dst, send, recv, j).start()
            return 0

        lax.fori_loop(1, na, body, 0)

    def all_z(src, dst, send, recv):
        def body(j, _):
            z_copy(src, dst, send, recv, j).start()
            return 0

        lax.fori_loop(0, nz - 1, body, 0)

    def arrived(name, ref, sem, n):
        part = ref.at[pl.ds(0, n)]
        with jax.named_scope(name):
            pltpu.make_async_copy(part, part, sem).wait()

    def by_group(perm, rows):
        return moved(perm[...], rows).reshape(na, OWN * nz, -1)

    def by_ring(perm, rows):
        return moved(perm[...], rows).reshape(nz, OWN * na, -1)

    for copy in raw_copies(0):
        copy.wait()
    s2[0] = by_ring(nat_z, raw[0])
    zr[0, z] = s2[0, z]
    with jax.named_scope("greet"):
        pl.semaphore_wait(barrier, (nz - 1) + (na - 1))
    all_z(s2.at[0], zr.at[0], z_send.at[0], z_recv.at[0])
    for k in range(1, chunks):
        for copy in raw_copies(k):
            copy.wait()
        s1[k] = by_group(split_a, raw[k])
        all_a(s1.at[k], ar.at[k], a_send.at[k], a_recv.at[k])
        ar[k, a] = s1[k, a]
    for k in range(1, chunks):
        arrived(f"a{k}", ar.at[k], a_recv.at[k], na - 1)
        s2[k] = by_ring(split_z, ar[k].reshape(members, CHUNK))
        all_z(s2.at[k], zr.at[k], z_send.at[k], z_recv.at[k])
        zr[k, z] = s2[k, z]

    arrived("z0", zr.at[0], z_recv.at[0], nz - 1)
    s1[0] = by_group(back_z, zr[0].reshape(members, CHUNK))
    all_a(s1.at[0], ar.at[0], a_send.at[0], a_recv.at[0])
    ar[0, a] = s1[0, a]

    for copy in row_copies:
        copy.wait()
    lines = lines_ref[0]
    eye = (
        lax.broadcasted_iota(jnp.int32, (members, members), 0)
        == lax.broadcasted_iota(jnp.int32, (members, members), 1)
    )
    identity = jnp.where(eye, f32(1.0), f32(0.0))
    gram[...] = f32(members - 1) * identity
    pull[...] = jnp.zeros_like(pull)
    for k in (*range(1, obs_chunks - 1), 0, obs_chunks - 1):
        if k == 0:
            arrived("a0", ar.at[0], a_recv.at[0], na - 1)
            values = jnp.dot(
                split_z[...], ar[0].reshape(members, CHUNK), preferred_element_type=f32
            )
        else:
            arrived(f"z{k}", zr.at[k], z_recv.at[k], nz - 1)
            values = zr[k].reshape(members, CHUNK).astype(f32)
        deviat = values - jnp.mean(values, axis=0, keepdims=True)
        row_ids = k * CHUNK + lax.broadcasted_iota(jnp.int32, (1, CHUNK), 1)
        cols = pl.ds(k * CHUNK, CHUNK)
        weights = jnp.where(row_ids < lines, prec_ref[:, cols], f32(0.0))
        weighted = deviat * weights
        gram[...] += lax.dot_general(
            weighted, deviat, (((1,), (1,)), ((), ())), precision=highest,
            preferred_element_type=f32,
        )
        pull[...] += jnp.sum(weighted * dep_ref[:, cols], axis=1, keepdims=True)

    def dot(p, q):
        return jnp.dot(p, q, precision=highest, preferred_element_type=f32)

    system = gram[...]
    scale = jnp.sqrt(jnp.sum(jnp.sum(system * system, axis=1, keepdims=True), axis=0, keepdims=True))
    itr[...] = system / scale
    root[...] = identity
    for sweep in range(ITERS):
        if sweep == 0:
            factor = 1.5 * identity - 0.5 * itr[...]
            root[...] = factor
        else:
            factor = 1.5 * identity - 0.5 * dot(root[...], itr[...])
            root[...] = dot(factor, root[...])
        if sweep < ITERS - 1:
            itr[...] = dot(itr[...], factor)

    inv_root = root[...]
    inner = jnp.sum(inv_root * pull[...], axis=0, keepdims=True)
    shift = jnp.sum(inv_root * inner, axis=1, keepdims=True) / scale
    shift = jnp.sum(jnp.where(eye, shift, f32(0.0)), axis=0, keepdims=True)
    transform = (math.sqrt(members - 1) / jnp.sqrt(scale)) * inv_root + shift

    arrived("zprior", zr.at[obs_chunks], z_recv.at[obs_chunks], nz - 1)
    quantities = zr[obs_chunks].reshape(members, CHUNK).astype(f32)
    center = jnp.mean(quantities, axis=0, keepdims=True)
    spread = quantities - center

    def result(half):
        cols = slice(half * HALF, (half + 1) * HALF)
        return (center[:, cols] + dot(transform, spread[:, cols])).astype(bf16)

    s3[0] = result(0).reshape(nz, OWN * na, HALF)
    all_z(s3.at[0], zb.at[0], zb_send.at[0], zb_recv.at[0])
    zb[0, z] = s3[0, z]
    s4[1] = by_group(back_z, result(1))
    all_a(s4.at[1], ab.at[1], ab_send.at[1], ab_recv.at[1])
    ab[1, a] = s4[1, a]
    arrived("aback1", ab.at[1], ab_recv.at[1], na - 1)
    s3[1] = by_ring(split_z, ab[1].reshape(members, HALF))
    all_z(s3.at[1], zb.at[1], zb_send.at[1], zb_recv.at[1])
    zb[1, z] = s3[1, z]
    arrived("zback0", zb.at[0], zb_recv.at[0], nz - 1)
    s4[0] = by_group(back_z, zb[0].reshape(members, HALF))
    all_a(s4.at[0], ab.at[0], ab_send.at[0], ab_recv.at[0])
    ab[0, a] = s4[0, a]

    def put(half, rows):
        out_ref[:, :, half * HALF : (half + 1) * HALF] = rows.reshape(OWN, patches, HALF)

    arrived("zback1", zb.at[1], zb_recv.at[1], nz - 1)
    put(1, moved(z_nat[...], zb[1].reshape(members, HALF)))
    arrived("aback0", ab.at[0], ab_recv.at[0], na - 1)
    put(0, moved(back_a[...], ab[0].reshape(members, HALF)))

    for k in range(chunks):
        arrived("sent", s1.at[k], a_send.at[k], na - 1)
        arrived("sent", s2.at[k], z_send.at[k], nz - 1)
    for half in range(2):
        arrived("sent", s3.at[half], zb_send.at[half], nz - 1)
        arrived("sent", s4.at[half], ab_send.at[half], na - 1)


def solution(mesh):
    nx, nz, nc = 4, 16, 2
    split = Mesh(mesh.devices.reshape(nx, nz, nc, mesh.shape["grp"]), ("x", "z", "c", "grp"))
    na = nx * nc
    members = OWN * na * nz

    def local(prior_members, mapped_prior, departure, precision_factor, measured_lines):
        chunks = mapped_prior.shape[2] // CHUNK + 1
        square = pltpu.VMEM((members, members), f32)
        perm = pltpu.VMEM((members, members), bf16)
        by_a = (na, OWN * nz, CHUNK)
        by_z = (nz, OWN * na, CHUNK)
        dma = pltpu.SemaphoreType.DMA
        return pl.pallas_call(
            functools.partial(kernel, nx, nz, nc),
            out_shape=jax.ShapeDtypeStruct(prior_members.shape, bf16),
            in_specs=[
                pl.BlockSpec(memory_space=pltpu.HBM),
                pl.BlockSpec(memory_space=pltpu.HBM),
                pl.BlockSpec(memory_space=pltpu.HBM),
                pl.BlockSpec(memory_space=pltpu.HBM),
                pl.BlockSpec(memory_space=pltpu.SMEM),
            ],
            out_specs=pl.BlockSpec(memory_space=pltpu.VMEM),
            scratch_shapes=[
                pltpu.VMEM((chunks, members, CHUNK), bf16),
                pltpu.VMEM(departure.shape, f32),
                pltpu.VMEM(precision_factor.shape, f32),
                perm, perm, perm, perm, perm, perm,
                pltpu.VMEM((chunks, *by_a), bf16),
                pltpu.VMEM((chunks, *by_a), bf16),
                pltpu.VMEM((chunks, *by_z), bf16),
                pltpu.VMEM((chunks, *by_z), bf16),
                pltpu.VMEM((2, nz, OWN * na, HALF), bf16),
                pltpu.VMEM((2, nz, OWN * na, HALF), bf16),
                pltpu.VMEM((2, na, OWN * nz, HALF), bf16),
                pltpu.VMEM((2, na, OWN * nz, HALF), bf16),
                square,
                pltpu.VMEM((members, 1), f32),
                square,
                square,
                dma((chunks, OWN)),
                dma((2,)),
                dma((chunks,)), dma((chunks,)),
                dma((chunks,)), dma((chunks,)),
                dma((2,)), dma((2,)), dma((2,)), dma((2,)),
            ],
            compiler_params=pltpu.CompilerParams(
                collective_id=0, has_side_effects=True, vmem_limit_bytes=48 << 20
            ),
        )(
            *(
                pltpu.with_memory_space_constraint(array, pltpu.HBM)
                for array in (prior_members, mapped_prior, departure, precision_factor)
            ),
            measured_lines,
        )

    return jax.shard_map(
        local,
        mesh=split,
        in_specs=(
            P(MEM, "grp", None),
            P(MEM, "grp", None),
            P(GRP_MEM, None),
            P(GRP_MEM, None),
            P(GRP_MEM),
        ),
        out_specs=P(MEM, "grp", None),
        check_vma=False,
    )
```

```python
import functools
import math

import jax
import jax.numpy as jnp
from jax import lax
from jax.experimental import pallas as pl
from jax.experimental.pallas import tpu as pltpu
from jax.sharding import Mesh
from jax.sharding import PartitionSpec as P

ITERS = 5
OWN = 2
CHUNK = 256
HALF = CHUNK // 2
MEM = ("x", "z", "c")
GRP_MEM = ("grp", "x", "z", "c")
MESH_ID = pl.DeviceIdType.MESH

f32 = jnp.float32
bf16 = jnp.bfloat16


def one_hot(rows, source_of):
    out_row = lax.broadcasted_iota(jnp.int32, (rows, rows), 0)
    in_row = lax.broadcasted_iota(jnp.int32, (rows, rows), 1)
    return jnp.where(in_row == source_of(out_row), f32(1.0), f32(0.0)).astype(bf16)


def moved(perm, rows):
    return jnp.dot(perm, rows, preferred_element_type=f32).astype(bf16)


def halves(value):
    high = value.astype(bf16)
    return high, (value - high.astype(f32)).astype(bf16)


def product(left, right, contract=1, against=0):
    def dot(p, q):
        return lax.dot_general(
            p, q, (((contract,), (against,)), ((), ())), preferred_element_type=f32
        )

    return dot(left[0], right[0]) + (dot(left[0], right[1]) + dot(left[1], right[0]))


def kernel(
    nx, nz, nc,
    prior_hbm, mapped_hbm, dep_hbm, prec_hbm, lines_ref, out_ref,
    raw, dep_ref, prec_ref,
    split_a, split_z, back_z, back_a, nat_z, z_nat,
    s1, ar, s2, zr, s2p, zrp, s3, zb, s4, ab, gram, pull,
    raw_sem, row_sem, far, a_send, a_recv, z_send, z_recv,
    p_send, p_recv, zb_send, zb_recv, ab_send, ab_recv,
):
    na = nx * nc
    members = OWN * na * nz
    obs_chunks = mapped_hbm.shape[2] // CHUNK
    chunks = obs_chunks + 1
    patches = nx * nz * nc
    hop = max(1, 3 * nz // 16)
    near = nz // 2 - hop
    x, z, c = lax.axis_index("x"), lax.axis_index("z"), lax.axis_index("c")
    a = x * nc + c

    barrier = pltpu.get_barrier_semaphore()

    def signal_z(sem, step):
        pl.semaphore_signal(
            sem, inc=1, device_id={"z": lax.rem(z + nz + step, nz)}, device_id_type=MESH_ID
        )

    def greet_z(j, _):
        signal_z(barrier, near - j)
        signal_z(barrier, j - near)
        return 0

    def greet_a(j, _):
        t = lax.rem(a + j, na)
        pl.semaphore_signal(
            barrier, inc=1, device_id={"x": t // nc, "c": lax.rem(t, nc)}, device_id_type=MESH_ID
        )
        return 0

    lax.fori_loop(0, near, greet_z, 0)
    lax.fori_loop(1, na, greet_a, 0)

    def raw_copies(k):
        if k < obs_chunks:
            src = lambda m: mapped_hbm.at[m, :, pl.ds(k * CHUNK, CHUNK)]
        else:
            src = lambda m: prior_hbm.at[m]
        return [
            pltpu.make_async_copy(src(m), raw.at[k, pl.ds(m * patches, patches)], raw_sem.at[k, m])
            for m in range(OWN)
        ]

    row_copies = [
        pltpu.make_async_copy(dep_hbm, dep_ref, row_sem.at[0]),
        pltpu.make_async_copy(prec_hbm, prec_ref, row_sem.at[1]),
    ]
    for k in range(chunks):
        for copy in raw_copies(k):
            copy.start()
    for copy in row_copies:
        copy.start()

    def natural(m, xi, zi, ci):
        return m * patches + xi * (nz * nc) + zi * nc + ci

    def of_natural(r):
        return r // patches, (r // (nz * nc)) % nx, (r // nc) % nz, r % nc

    def of_group(r):
        return r % OWN, r // (OWN * nz * nc), (r // OWN) % nz, (r // (OWN * nz)) % nc

    def of_ring(r):
        return r % OWN, (r // (OWN * nc)) % nx, r // (OWN * na), (r // OWN) % nc

    def group(m, xi, zi, ci):
        return ((xi * nc + ci) * nz + zi) * OWN + m

    def ring(m, xi, zi, ci):
        return ((zi * nx + xi) * nc + ci) * OWN + m

    def a_copy(src, dst, send, recv, j):
        t = lax.rem(a + j, na)
        return pltpu.make_async_remote_copy(
            src_ref=src.at[t], dst_ref=dst.at[a], send_sem=send, recv_sem=recv,
            device_id={"x": t // nc, "c": lax.rem(t, nc)}, device_id_type=MESH_ID,
        )

    def z_copy(src, dst, send, recv, step):
        t = lax.rem(z + nz + step, nz)
        return pltpu.make_async_remote_copy(
            src_ref=src.at[t], dst_ref=dst.at[z], send_sem=send, recv_sem=recv,
            device_id={"z": t}, device_id_type=MESH_ID,
        )

    def all_a(src, dst, send, recv):
        def body(j, _):
            a_copy(src, dst, send, recv, j).start()
            return 0

        lax.fori_loop(1, na, body, 0)

    def ring_steps(most, least, *copy_args):
        def body(j, _):
            z_copy(*copy_args, most - j).start()
            z_copy(*copy_args, j - most).start()
            return 0

        lax.fori_loop(0, most - least + 1, body, 0)

    def opposite(*copy_args):
        z_copy(*copy_args, nz // 2).start()

    def all_z(*copy_args):
        opposite(*copy_args)
        ring_steps(nz // 2 - 1, 1, *copy_args)

    def arrived(name, ref, sem, n):
        part = ref.at[pl.ds(0, n)]
        with jax.named_scope(name):
            pltpu.make_async_copy(part, part, sem).wait()

    def by_group(perm, rows):
        return moved(perm[...], rows).reshape(na, OWN * nz, -1)

    def by_ring(perm, rows):
        return moved(perm[...], rows).reshape(nz, OWN * na, -1)

    def send_group(k):
        for copy in raw_copies(k):
            copy.wait()
        s1[k] = by_group(split_a, raw[k])
        all_a(s1.at[k], ar.at[k], a_send.at[k], a_recv.at[k])
        ar[k, a] = s1[k, a]

    nat_z[...] = one_hot(members, lambda r: natural(*of_ring(r)))
    for copy in raw_copies(0):
        copy.wait()
    s2[0] = by_ring(nat_z, raw[0])
    zr[0, z] = s2[0, z]
    split_a[...] = one_hot(members, lambda r: natural(*of_group(r)))
    first = (s2.at[0], zr.at[0], z_send.at[0], z_recv.at[0])
    with jax.named_scope("greet"):
        pl.semaphore_wait(barrier, 2 * near + na - 1)
    signal_z(far, hop)
    signal_z(far, -hop)
    ring_steps(near, 1, *first)
    for k in range(1, chunks - 2):
        send_group(k)
    with jax.named_scope("far"):
        pl.semaphore_wait(far, 2)
    opposite(*first)
    if near + 1 < nz // 2:
        ring_steps(nz // 2 - 1, near + 1, *first)
    for k in range(chunks - 2, chunks):
        send_group(k)
    split_z[...] = one_hot(members, lambda r: group(*of_ring(r)))
    back_z[...] = one_hot(members, lambda r: ring(*of_group(r)))
    for k in range(1, chunks):
        arrived(f"a{k}", ar.at[k], a_recv.at[k], na - 1)
        rows = ar[k].reshape(members, CHUNK)
        if k < obs_chunks:
            s2[k] = by_ring(split_z, rows)
            all_z(s2.at[k], zr.at[k], z_send.at[k], z_recv.at[k])
            zr[k, z] = s2[k, z]
        else:
            rows = moved(split_z[...], rows)
            for h in range(2):
                s2p[h] = rows[:, h * HALF : (h + 1) * HALF].reshape(nz, OWN * na, HALF)
                all_z(s2p.at[h], zrp.at[h], p_send.at[h], p_recv.at[h])
                zrp[h, z] = s2p[h, z]
    back_a[...] = one_hot(members, lambda r: group(*of_natural(r)))
    z_nat[...] = one_hot(members, lambda r: ring(*of_natural(r)))

    arrived("z0", zr.at[0], z_recv.at[0], nz - 1)
    s1[0] = by_group(back_z, zr[0].reshape(members, CHUNK))
    all_a(s1.at[0], ar.at[0], a_send.at[0], a_recv.at[0])
    ar[0, a] = s1[0, a]

    for copy in row_copies:
        copy.wait()
    lines = lines_ref[0]
    eye = (
        lax.broadcasted_iota(jnp.int32, (members, members), 0)
        == lax.broadcasted_iota(jnp.int32, (members, members), 1)
    )
    gram[...] = jnp.where(eye, f32(members - 1), f32(0.0))
    pull[...] = jnp.zeros_like(pull)
    for k in (*range(1, obs_chunks - 1), 0, obs_chunks - 1):
        if k == 0:
            arrived("a0", ar.at[0], a_recv.at[0], na - 1)
            values = jnp.dot(
                split_z[...], ar[0].reshape(members, CHUNK), preferred_element_type=f32
            )
        else:
            arrived(f"z{k}", zr.at[k], z_recv.at[k], nz - 1)
            values = zr[k].reshape(members, CHUNK).astype(f32)
        with jax.named_scope("gram"):
            deviat = values - jnp.mean(values, axis=0, keepdims=True)
            row_ids = k * CHUNK + lax.broadcasted_iota(jnp.int32, (1, CHUNK), 1)
            cols = pl.ds(k * CHUNK, CHUNK)
            weights = jnp.where(row_ids < lines, prec_ref[:, cols], f32(0.0))
            weighted = deviat * weights
            gram[...] += product(halves(weighted), halves(deviat), 1, 1)
            pull[...] += jnp.sum(weighted * dep_ref[:, cols], axis=1, keepdims=True)

    with jax.named_scope("newton"):
        system = gram[...]
        scale = jnp.sqrt(
            jnp.sum(jnp.sum(system * system, axis=1, keepdims=True), axis=0, keepdims=True)
        )
        identity = jnp.where(eye, f32(1.5), f32(0.0))
        iterate = system / scale
        root = identity - 0.5 * iterate
        factor_halves = halves(root)
        root_halves = factor_halves
        iterate_halves = halves(product(halves(iterate), factor_halves))
        for sweep in range(1, ITERS):
            factor_halves = halves(identity - 0.5 * product(root_halves, iterate_halves))
            root = product(factor_halves, root_halves)
            if sweep < ITERS - 1:
                iterate_halves = halves(product(iterate_halves, factor_halves))
                root_halves = halves(root)

        inner = jnp.sum(root * pull[...], axis=0, keepdims=True)
        shift = jnp.sum(root * inner, axis=1, keepdims=True) / scale
        shift = jnp.sum(jnp.where(eye, shift, f32(0.0)), axis=0, keepdims=True)
        transform = halves((math.sqrt(members - 1) / jnp.sqrt(scale)) * root + shift)

    def result(h):
        arrived(f"p{h}", zrp.at[h], p_recv.at[h], nz - 1)
        quantities = zrp[h].reshape(members, HALF).astype(f32)
        center = jnp.mean(quantities, axis=0, keepdims=True)
        return (center + product(transform, halves(quantities - center))).astype(bf16)

    s3[0] = result(0).reshape(nz, OWN * na, HALF)
    all_z(s3.at[0], zb.at[0], zb_send.at[0], zb_recv.at[0])
    zb[0, z] = s3[0, z]
    s4[1] = by_group(back_z, result(1))
    all_a(s4.at[1], ab.at[1], ab_send.at[1], ab_recv.at[1])
    ab[1, a] = s4[1, a]
    arrived("aback1", ab.at[1], ab_recv.at[1], na - 1)
    s3[1] = by_ring(split_z, ab[1].reshape(members, HALF))
    all_z(s3.at[1], zb.at[1], zb_send.at[1], zb_recv.at[1])
    zb[1, z] = s3[1, z]
    arrived("zback0", zb.at[0], zb_recv.at[0], nz - 1)
    s4[0] = by_group(back_z, zb[0].reshape(members, HALF))
    all_a(s4.at[0], ab.at[0], ab_send.at[0], ab_recv.at[0])
    ab[0, a] = s4[0, a]

    def put(half, rows):
        out_ref[:, :, half * HALF : (half + 1) * HALF] = rows.reshape(OWN, patches, HALF)

    arrived("aback0", ab.at[0], ab_recv.at[0], na - 1)
    put(0, moved(back_a[...], ab[0].reshape(members, HALF)))
    arrived("zback1", zb.at[1], zb_recv.at[1], nz - 1)
    put(1, moved(z_nat[...], zb[1].reshape(members, HALF)))

    for k in range(chunks):
        arrived("sent", s1.at[k], a_send.at[k], na - 1)
        if k < obs_chunks:
            arrived("sent", s2.at[k], z_send.at[k], nz - 1)
    for half in range(2):
        arrived("sent", s2p.at[half], p_send.at[half], nz - 1)
        arrived("sent", s3.at[half], zb_send.at[half], nz - 1)
        arrived("sent", s4.at[half], ab_send.at[half], na - 1)


def solution(mesh):
    nx, nz, nc = 4, 16, 2
    split = Mesh(mesh.devices.reshape(nx, nz, nc, mesh.shape["grp"]), ("x", "z", "c", "grp"))
    na = nx * nc
    members = OWN * na * nz

    def local(prior_members, mapped_prior, departure, precision_factor, measured_lines):
        chunks = mapped_prior.shape[2] // CHUNK + 1
        perm = pltpu.VMEM((members, members), bf16)
        by_a = (na, OWN * nz)
        by_z = (nz, OWN * na)
        dma = pltpu.SemaphoreType.DMA
        return pl.pallas_call(
            functools.partial(kernel, nx, nz, nc),
            out_shape=jax.ShapeDtypeStruct(prior_members.shape, bf16),
            in_specs=[
                pl.BlockSpec(memory_space=pltpu.HBM),
                pl.BlockSpec(memory_space=pltpu.HBM),
                pl.BlockSpec(memory_space=pltpu.HBM),
                pl.BlockSpec(memory_space=pltpu.HBM),
                pl.BlockSpec(memory_space=pltpu.SMEM),
            ],
            out_specs=pl.BlockSpec(memory_space=pltpu.VMEM),
            scratch_shapes=[
                pltpu.VMEM((chunks, members, CHUNK), bf16),
                pltpu.VMEM(departure.shape, f32),
                pltpu.VMEM(precision_factor.shape, f32),
                perm, perm, perm, perm, perm, perm,
                pltpu.VMEM((chunks, *by_a, CHUNK), bf16),
                pltpu.VMEM((chunks, *by_a, CHUNK), bf16),
                pltpu.VMEM((chunks - 1, *by_z, CHUNK), bf16),
                pltpu.VMEM((chunks - 1, *by_z, CHUNK), bf16),
                pltpu.VMEM((2, *by_z, HALF), bf16),
                pltpu.VMEM((2, *by_z, HALF), bf16),
                pltpu.VMEM((2, *by_z, HALF), bf16),
                pltpu.VMEM((2, *by_z, HALF), bf16),
                pltpu.VMEM((2, *by_a, HALF), bf16),
                pltpu.VMEM((2, *by_a, HALF), bf16),
                pltpu.VMEM((members, members), f32),
                pltpu.VMEM((members, 1), f32),
                dma((chunks, OWN)),
                dma((2,)),
                pltpu.SemaphoreType.REGULAR,
                dma((chunks,)), dma((chunks,)),
                dma((chunks - 1,)), dma((chunks - 1,)),
                dma((2,)), dma((2,)),
                dma((2,)), dma((2,)),
                dma((2,)), dma((2,)),
            ],
            compiler_params=pltpu.CompilerParams(
                collective_id=0, has_side_effects=True, vmem_limit_bytes=48 << 20
            ),
        )(
            *(
                pltpu.with_memory_space_constraint(array, pltpu.HBM)
                for array in (
                    prior_members, mapped_prior, departure, precision_factor,
                )
            ),
            measured_lines,
        )

    return jax.shard_map(
        local,
        mesh=split,
        in_specs=(
            P(MEM, "grp", None),
            P(MEM, "grp", None),
            P(GRP_MEM, None),
            P(GRP_MEM, None),
            P(GRP_MEM),
        ),
        out_specs=P(MEM, "grp", None),
        check_vma=False,
    )
```

```python
import functools
import math

import jax
import jax.numpy as jnp
from jax import lax
from jax.experimental import pallas as pl
from jax.experimental.pallas import tpu as pltpu
from jax.sharding import Mesh
from jax.sharding import PartitionSpec as P

ITERS = 5
OWN = 2
CHUNK = 256
HALF = CHUNK // 2
RING_FIRST = 2
MEM = ("x", "z", "c")
GRP_MEM = ("grp", "x", "z", "c")
MESH_ID = pl.DeviceIdType.MESH

f32 = jnp.float32
bf16 = jnp.bfloat16


def one_hot(rows, source_of):
    out_row = lax.broadcasted_iota(jnp.int32, (rows, rows), 0)
    in_row = lax.broadcasted_iota(jnp.int32, (rows, rows), 1)
    return jnp.where(in_row == source_of(out_row), f32(1.0), f32(0.0)).astype(bf16)


def moved(perm, rows):
    return jnp.dot(perm, rows, preferred_element_type=f32).astype(bf16)


def halves(value):
    high = value.astype(bf16)
    return high, (value - high.astype(f32)).astype(bf16)


def product(left, right, contract=1, against=0):
    def dot(p, q):
        return lax.dot_general(
            p, q, (((contract,), (against,)), ((), ())), preferred_element_type=f32
        )

    return dot(left[0], right[0]) + (dot(left[0], right[1]) + dot(left[1], right[0]))


def kernel(
    nx, nz, nc,
    prior_hbm, mapped_hbm, dep_hbm, prec_hbm, lines_ref, out_ref,
    raw, dep_ref, prec_ref,
    split_a, split_z, back_z, back_a, nat_z, z_nat,
    s1, ar, s2, zr, s2p, zrp, s3, zb, s4, ab, s5, db, gram, pull,
    raw_sem, row_sem, far, a_send, a_recv, z_send, z_recv,
    p_send, p_recv, zb_send, zb_recv, ab_send, ab_recv, db_sem,
):
    na = nx * nc
    members = OWN * na * nz
    obs_chunks = mapped_hbm.shape[2] // CHUNK
    chunks = obs_chunks + 1
    patches = nx * nz * nc
    near = max(1, nz // 4)
    levels = nz // (2 * near)
    x, z, c = lax.axis_index("x"), lax.axis_index("z"), lax.axis_index("c")
    a = x * nc + c

    barrier = pltpu.get_barrier_semaphore()

    def signal_z(sem, step):
        pl.semaphore_signal(
            sem, inc=1, device_id={"z": lax.rem(z + nz + step, nz)}, device_id_type=MESH_ID
        )

    def greet_a(j, _):
        t = lax.rem(a + j, na)
        pl.semaphore_signal(
            barrier, inc=1, device_id={"x": t // nc, "c": lax.rem(t, nc)}, device_id_type=MESH_ID
        )
        return 0

    def raw_copies(k):
        if k < obs_chunks:
            src = lambda m: mapped_hbm.at[m, :, pl.ds(k * CHUNK, CHUNK)]
        else:
            src = lambda m: prior_hbm.at[m]
        return [
            pltpu.make_async_copy(src(m), raw.at[k, pl.ds(m * patches, patches)], raw_sem.at[k, m])
            for m in range(OWN)
        ]

    row_copies = [
        pltpu.make_async_copy(dep_hbm, dep_ref, row_sem.at[0]),
        pltpu.make_async_copy(prec_hbm, prec_ref, row_sem.at[1]),
    ]
    for copy in raw_copies(0):
        copy.start()
    for step in range(near, 0, -1):
        signal_z(barrier, step)
        signal_z(barrier, -step)
    lax.fori_loop(1, na, greet_a, 0)
    for k in range(1, chunks):
        for copy in raw_copies(k):
            copy.start()
    for copy in row_copies:
        copy.start()

    def natural(m, xi, zi, ci):
        return m * patches + xi * (nz * nc) + zi * nc + ci

    def of_natural(r):
        return r // patches, (r // (nz * nc)) % nx, (r // nc) % nz, r % nc

    def of_group(r):
        return r % OWN, r // (OWN * nz * nc), (r // OWN) % nz, (r // (OWN * nz)) % nc

    def of_ring(r):
        return r % OWN, (r // (OWN * nc)) % nx, r // (OWN * na), (r // OWN) % nc

    def group(m, xi, zi, ci):
        return ((xi * nc + ci) * nz + zi) * OWN + m

    def ring(m, xi, zi, ci):
        return ((zi * nx + xi) * nc + ci) * OWN + m

    def a_copy(src, dst, send, recv, j):
        t = lax.rem(a + j, na)
        return pltpu.make_async_remote_copy(
            src_ref=src.at[t], dst_ref=dst.at[a], send_sem=send, recv_sem=recv,
            device_id={"x": t // nc, "c": lax.rem(t, nc)}, device_id_type=MESH_ID,
        )

    def z_copy(src, dst, send, recv, step):
        t = lax.rem(z + nz + step, nz)
        return pltpu.make_async_remote_copy(
            src_ref=src.at[t], dst_ref=dst.at[z], send_sem=send, recv_sem=recv,
            device_id={"z": t}, device_id_type=MESH_ID,
        )

    def all_a(src, dst, send, recv):
        def body(j, _):
            a_copy(src, dst, send, recv, j).start()
            return 0

        lax.fori_loop(1, na, body, 0)

    def ring_steps(most, least, *copy_args):
        def body(j, _):
            z_copy(*copy_args, most - j).start()
            z_copy(*copy_args, j - most).start()
            return 0

        lax.fori_loop(0, most - least + 1, body, 0)

    def ring_part(level, *copy_args):
        most = near * (level + 1)
        if most == nz // 2:
            z_copy(*copy_args, most).start()
            most -= 1
        if most > near * level:
            ring_steps(most, near * level + 1, *copy_args)

    def all_z(*copy_args):
        z_copy(*copy_args, nz // 2).start()
        ring_steps(nz // 2 - 1, 1, *copy_args)

    def all_a(src, dst, send, recv):
        def body(j, _):
            a_copy(src, dst, send, recv, j).start()
            return 0

        lax.fori_loop(1, na, body, 0)

    def ring_steps(most, least, *copy_args):
        def body(j, _):
            z_copy(*copy_args, most - j).start()
            z_copy(*copy_args, j - most).start()
            return 0

        lax.fori_loop(0, most - least + 1, body, 0)

    def ring_part(level, *copy_args):
        most = near * (level + 1)
        if most == nz // 2:
            z_copy(*copy_args, most).start()
            most -= 1
        if most > near * level:
            ring_steps(most, near * level + 1, *copy_args)

    def all_z(*copy_args):
        z_copy(*copy_args, nz // 2).start()
        ring_steps(nz // 2 - 1, 1, *copy_args)

    first, last = nz // 2 - nz // 8, nz // 2 + nz // 8

    def served_first(src, dst, send, recv):
        for j in range(last - first + 1):
            t = nz // 2 + ((j + 1) // 2) * (1 if j % 2 else -1)

            @pl.when(z != t)
            def _():
                z_copy(src, dst, send, recv, t - z).start()

    def served_later(*copy_args):
        def one(step):
            t = lax.rem(z + nz + step, nz)

            @pl.when(jnp.logical_or(t < first, t > last))
            def _():
                z_copy(*copy_args, step).start()

        def body(j, _):
            one(nz // 2 - 1 - j)
            one(j - nz // 2 + 1)
            return 0

        one(nz // 2)
        lax.fori_loop(0, nz // 2 - 1, body, 0)

    def arrived(name, ref, sem, n):
        part = ref.at[pl.ds(0, n)]
        with jax.named_scope(name):
            pltpu.make_async_copy(part, part, sem).wait()

    def by_group(perm, rows):
        return moved(perm[...], rows).reshape(na, OWN * nz, -1)

    def by_ring(perm, rows):
        return moved(perm[...], rows).reshape(nz, OWN * na, -1)

    def send_group(k):
        for copy in raw_copies(k):
            copy.wait()
        s1[k] = by_group(split_a, raw[k])
        all_a(s1.at[k], ar.at[k], a_send.at[k], a_recv.at[k])
        ar[k, a] = s1[k, a]

    def send_group(k):
        for copy in raw_copies(k):
            copy.wait()
        s1[k] = by_group(split_a, raw[k])
        all_a(s1.at[k], ar.at[k], a_send.at[k], a_recv.at[k])
        ar[k, a] = s1[k, a]

    def ring_args(k):
        return s2.at[k], zr.at[k], z_send.at[k], z_recv.at[k]

    def make_ring(k):
        for copy in raw_copies(k):
            copy.wait()
        s2[k] = by_ring(nat_z, raw[k])
        zr[k, z] = s2[k, z]

    nat_z[...] = one_hot(members, lambda r: natural(*of_ring(r)))
    make_ring(0)
    with jax.named_scope("greet"):
        pl.semaphore_wait(barrier, 2 * near + na - 1)
    for level in range(levels):
        if level:
            with jax.named_scope(f"far{level}"):
                pl.semaphore_wait(far.at[level - 1], 2)
        if level < levels - 1:
            signal_z(far.at[level], near)
            signal_z(far.at[level], -near)
        ring_part(level, *ring_args(0))
        if level == 0:
            for k in range(1, RING_FIRST):
                make_ring(k)
                ring_part(0, *ring_args(k))
            split_a[...] = one_hot(members, lambda r: natural(*of_group(r)))
        else:
            for k in range(1, RING_FIRST):
                ring_part(level, *ring_args(k))
        if RING_FIRST + level < chunks:
            send_group(RING_FIRST + level)
    for k in range(RING_FIRST + levels, chunks):
        send_group(k)
    split_z[...] = one_hot(members, lambda r: group(*of_ring(r)))
    for k in range(RING_FIRST, chunks):
        arrived(f"a{k}", ar.at[k], a_recv.at[k], na - 1)
        rows = ar[k].reshape(members, CHUNK)
        if k < obs_chunks:
            s2[k] = by_ring(split_z, rows)
            all_z(*ring_args(k))
            zr[k, z] = s2[k, z]
        else:
            rows = moved(split_z[...], rows)
            for h in range(2):
                s2p[h] = rows[:, h * HALF : (h + 1) * HALF].reshape(nz, OWN * na, HALF)
                all_z(s2p.at[h], zrp.at[h], p_send.at[h], p_recv.at[h])
                zrp[h, z] = s2p[h, z]
    back_z[...] = one_hot(members, lambda r: ring(*of_group(r)))
    back_a[...] = one_hot(members, lambda r: group(*of_natural(r)))
    z_nat[...] = one_hot(members, lambda r: ring(*of_natural(r)))

    for k in range(RING_FIRST):
        arrived(f"z{k}", zr.at[k], z_recv.at[k], nz - 1)
        s1[k] = by_group(back_z, zr[k].reshape(members, CHUNK))
        all_a(s1.at[k], ar.at[k], a_send.at[k], a_recv.at[k])
        ar[k, a] = s1[k, a]

    for copy in row_copies:
        copy.wait()
    lines = lines_ref[0]
    eye = (
        lax.broadcasted_iota(jnp.int32, (members, members), 0)
        == lax.broadcasted_iota(jnp.int32, (members, members), 1)
    )
    gram[...] = jnp.where(eye, f32(members - 1), f32(0.0))
    pull[...] = jnp.zeros_like(pull)
    for k in (*range(RING_FIRST, obs_chunks - 1), *range(RING_FIRST), obs_chunks - 1):
        if k < RING_FIRST:
            arrived(f"a{k}", ar.at[k], a_recv.at[k], na - 1)
            values = jnp.dot(
                split_z[...], ar[k].reshape(members, CHUNK), preferred_element_type=f32
            )
        else:
            arrived(f"z{k}", zr.at[k], z_recv.at[k], nz - 1)
            values = zr[k].reshape(members, CHUNK).astype(f32)
        with jax.named_scope("gram"):
            deviat = values - jnp.mean(values, axis=0, keepdims=True)
            row_ids = k * CHUNK + lax.broadcasted_iota(jnp.int32, (1, CHUNK), 1)
            cols = pl.ds(k * CHUNK, CHUNK)
            weights = jnp.where(row_ids < lines, prec_ref[:, cols], f32(0.0))
            weighted = deviat * weights
            gram[...] += product(halves(weighted), halves(deviat), 1, 1)
            pull[...] += jnp.sum(weighted * dep_ref[:, cols], axis=1, keepdims=True)

    with jax.named_scope("newton"):
        system = gram[...]
        scale = jnp.sqrt(
            jnp.sum(jnp.sum(system * system, axis=1, keepdims=True), axis=0, keepdims=True)
        )
        identity = jnp.where(eye, f32(1.5), f32(0.0))
        iterate = system / scale
        root = identity - 0.5 * iterate
        factor_halves = halves(root)
        root_halves = factor_halves
        iterate_halves = halves(product(halves(iterate), factor_halves))
        for sweep in range(1, ITERS):
            factor_halves = halves(identity - 0.5 * product(root_halves, iterate_halves))
            root = product(factor_halves, root_halves)
            if sweep < ITERS - 1:
                iterate_halves = halves(product(iterate_halves, factor_halves))
                root_halves = halves(root)

        inner = jnp.sum(root * pull[...], axis=0, keepdims=True)
        shift = jnp.sum(root * inner, axis=1, keepdims=True) / scale
        shift = jnp.sum(jnp.where(eye, shift, f32(0.0)), axis=0, keepdims=True)
        transform = (math.sqrt(members - 1) / jnp.sqrt(scale)) * root + shift
        transform = halves(transform)
        kept = 1.0 - jnp.sum(
            transform[0].astype(f32) + transform[1].astype(f32), axis=1, keepdims=True
        )

    def result(h, rows, kept):
        arrived(f"p{h}", zrp.at[h], p_recv.at[h], nz - 1)
        quantities = zrp[h].reshape(members, HALF)
        center = jnp.mean(quantities.astype(f32), axis=0, keepdims=True)
        spread = jnp.dot(rows[0], quantities, preferred_element_type=f32) + (
            jnp.dot(rows[1], quantities, preferred_element_type=f32)
        )
        return (spread + kept * center).astype(bf16)

    def group_back(h):
        all_a(s4.at[h], ab.at[h], ab_send.at[h], ab_recv.at[h])
        ab[h, a] = s4[h, a]

    def ring_back(h):
        all_z(s3.at[h], zb.at[h], zb_send.at[h], zb_recv.at[h])
        zb[h, z] = s3[h, z]

    def put(h, rows):
        out_ref[:, :, h * HALF : (h + 1) * HALF] = rows.reshape(OWN, patches, HALF)

    s3[0] = result(0, transform, kept).reshape(nz, OWN * na, HALF)
    ring_back(0)
    s5[...] = result(1, transform, kept).reshape(s5.shape)

    def straight(step):
        t = lax.rem(z + nz + step, nz)
        for j in range(na):
            g = lax.rem(a + j, na)

            def send():
                pltpu.make_async_remote_copy(
                    src_ref=s5.at[t * na + g], dst_ref=db.at[z * na + a],
                    send_sem=db_sem.at[0], recv_sem=db_sem.at[1],
                    device_id={"x": g // nc, "z": t, "c": lax.rem(g, nc)},
                    device_id_type=MESH_ID,
                ).start()

            if j or not isinstance(step, int) or step:
                send()

    def straight_both(j, _):
        straight(nz // 2 - 1 - j)
        straight(j - nz // 2 + 1)
        return 0

    straight(nz // 2)
    lax.fori_loop(0, nz // 2 - 1, straight_both, 0)
    straight(0)
    db[z * na + a] = s5[z * na + a]
    arrived("zback0", zb.at[0], zb_recv.at[0], nz - 1)
    s4[0] = by_group(back_z, zb[0].reshape(members, HALF))
    group_back(0)
    arrived("straight", db, db_sem.at[1], na * nz - 1)
    put(1, moved(z_nat[...], db[...].reshape(members, HALF)))
    arrived("aback0", ab.at[0], ab_recv.at[0], na - 1)
    put(0, moved(back_a[...], ab[0].reshape(members, HALF)))
    arrived("sent", s5, db_sem.at[0], na * nz - 1)

    for k in range(chunks):
        arrived("sent", s1.at[k], a_send.at[k], na - 1)
        if k < obs_chunks:
            arrived("sent", s2.at[k], z_send.at[k], nz - 1)
    arrived("sent", s3.at[0], zb_send.at[0], nz - 1)
    arrived("sent", s4.at[0], ab_send.at[0], na - 1)
    for half in range(2):
        arrived("sent", s2p.at[half], p_send.at[half], nz - 1)


def solution(mesh):
    nx, nz, nc = 4, 16, 2
    split = Mesh(mesh.devices.reshape(nx, nz, nc, mesh.shape["grp"]), ("x", "z", "c", "grp"))
    na = nx * nc
    members = OWN * na * nz

    def local(prior_members, mapped_prior, departure, precision_factor, measured_lines):
        chunks = mapped_prior.shape[2] // CHUNK + 1
        perm = pltpu.VMEM((members, members), bf16)
        by_a = (na, OWN * nz)
        by_z = (nz, OWN * na)
        dma = pltpu.SemaphoreType.DMA
        return pl.pallas_call(
            functools.partial(kernel, nx, nz, nc),
            out_shape=jax.ShapeDtypeStruct(prior_members.shape, bf16),
            in_specs=[
                pl.BlockSpec(memory_space=pltpu.HBM),
                pl.BlockSpec(memory_space=pltpu.HBM),
                pl.BlockSpec(memory_space=pltpu.HBM),
                pl.BlockSpec(memory_space=pltpu.HBM),
                pl.BlockSpec(memory_space=pltpu.SMEM),
            ],
            out_specs=pl.BlockSpec(memory_space=pltpu.VMEM),
            scratch_shapes=[
                pltpu.VMEM((chunks, members, CHUNK), bf16),
                pltpu.VMEM(departure.shape, f32),
                pltpu.VMEM(precision_factor.shape, f32),
                perm, perm, perm, perm, perm, perm,
                pltpu.VMEM((chunks, *by_a, CHUNK), bf16),
                pltpu.VMEM((chunks, *by_a, CHUNK), bf16),
                pltpu.VMEM((chunks - 1, *by_z, CHUNK), bf16),
                pltpu.VMEM((chunks - 1, *by_z, CHUNK), bf16),
                pltpu.VMEM((2, *by_z, HALF), bf16),
                pltpu.VMEM((2, *by_z, HALF), bf16),
                pltpu.VMEM((1, *by_z, HALF), bf16),
                pltpu.VMEM((1, *by_z, HALF), bf16),
                pltpu.VMEM((1, *by_a, HALF), bf16),
                pltpu.VMEM((1, *by_a, HALF), bf16),
                pltpu.VMEM((na * nz, OWN, HALF), bf16),
                pltpu.VMEM((na * nz, OWN, HALF), bf16),
                pltpu.VMEM((members, members), f32),
                pltpu.VMEM((members, 1), f32),
                dma((chunks, OWN)),
                dma((2,)),
                pltpu.SemaphoreType.REGULAR((3,)),
                dma((chunks,)), dma((chunks,)),
                dma((chunks - 1,)), dma((chunks - 1,)),
                dma((2,)), dma((2,)),
                dma((1,)), dma((1,)),
                dma((1,)), dma((1,)),
                dma((2,)),
            ],
            compiler_params=pltpu.CompilerParams(
                collective_id=0, has_side_effects=True, vmem_limit_bytes=48 << 20
            ),
        )(
            *(
                pltpu.with_memory_space_constraint(array, pltpu.HBM)
                for array in (
                    prior_members, mapped_prior, departure, precision_factor,
                )
            ),
            measured_lines,
        )

    return jax.shard_map(
        local,
        mesh=split,
        in_specs=(
            P(MEM, "grp", None),
            P(MEM, "grp", None),
            P(GRP_MEM, None),
            P(GRP_MEM, None),
            P(GRP_MEM),
        ),
        out_specs=P(MEM, "grp", None),
        check_vma=False,
    )
```

```python
import functools
import math

import jax
import jax.numpy as jnp
from jax import lax
from jax.experimental import pallas as pl
from jax.experimental.pallas import tpu as pltpu
from jax.sharding import Mesh
from jax.sharding import PartitionSpec as P

ITERS = 5
OWN = 2
CHUNK = 256
HALF = CHUNK // 2
RING_FIRST = 2
NEAR = 4
MEM = ("x", "z", "c")
GRP_MEM = ("grp", "x", "z", "c")
MESH_ID = pl.DeviceIdType.MESH

f32 = jnp.float32
bf16 = jnp.bfloat16


def one_hot(rows, source_of):
    out_row = lax.broadcasted_iota(jnp.int32, (rows, rows), 0)
    in_row = lax.broadcasted_iota(jnp.int32, (rows, rows), 1)
    return jnp.where(in_row == source_of(out_row), f32(1.0), f32(0.0)).astype(bf16)


def moved(perm, rows):
    return jnp.dot(perm, rows, preferred_element_type=f32).astype(bf16)


def halves(value):
    high = value.astype(bf16)
    return high, (value - high.astype(f32)).astype(bf16)


def product(left, right, contract=1, against=0):
    def dot(p, q):
        return lax.dot_general(
            p, q, (((contract,), (against,)), ((), ())), preferred_element_type=f32
        )

    return dot(left[0], right[0]) + (dot(left[0], right[1]) + dot(left[1], right[0]))


def kernel(
    nx, nz, nc,
    prior_hbm, mapped_hbm, dep_hbm, prec_hbm, lines_ref, out_ref,
    raw, dep_ref, prec_ref,
    split_a, split_z, back_z, nat_z, z_nat,
    s1, ar, s2, zr, s2p, zrp, s5, db, gram, pull,
    raw_sem, row_sem, far, a_send, a_recv, z_send, z_recv,
    p_send, p_recv, db_send, db_recv,
):
    na = nx * nc
    members = OWN * na * nz
    obs_chunks = mapped_hbm.shape[2] // CHUNK
    chunks = obs_chunks + 1
    patches = nx * nz * nc
    near = nz * NEAR // 16
    hop = nz // 2 - near
    x, z, c = lax.axis_index("x"), lax.axis_index("z"), lax.axis_index("c")
    a = x * nc + c

    barrier = pltpu.get_barrier_semaphore()

    def signal_z(sem, step):
        pl.semaphore_signal(
            sem, inc=1, device_id={"z": lax.rem(z + nz + step, nz)}, device_id_type=MESH_ID
        )

    def greet_a(j, _):
        t = lax.rem(a + j, na)
        pl.semaphore_signal(
            barrier, inc=1, device_id={"x": t // nc, "c": lax.rem(t, nc)}, device_id_type=MESH_ID
        )
        return 0

    def raw_copies(k):
        if k < obs_chunks:
            src = lambda m: mapped_hbm.at[m, :, pl.ds(k * CHUNK, CHUNK)]
        else:
            src = lambda m: prior_hbm.at[m]
        return [
            pltpu.make_async_copy(src(m), raw.at[k, pl.ds(m * patches, patches)], raw_sem.at[k, m])
            for m in range(OWN)
        ]

    row_copies = [
        pltpu.make_async_copy(dep_hbm, dep_ref, row_sem.at[0]),
        pltpu.make_async_copy(prec_hbm, prec_ref, row_sem.at[1]),
    ]
    for copy in raw_copies(0):
        copy.start()
    for step in range(near, 0, -1):
        signal_z(barrier, step)
        signal_z(barrier, -step)
    lax.fori_loop(1, na, greet_a, 0)
    for k in range(1, chunks):
        for copy in raw_copies(k):
            copy.start()
    for copy in row_copies:
        copy.start()

    def natural(m, xi, zi, ci):
        return m * patches + xi * (nz * nc) + zi * nc + ci

    def of_natural(r):
        return r // patches, (r // (nz * nc)) % nx, (r // nc) % nz, r % nc

    def of_group(r):
        return r % OWN, r // (OWN * nz * nc), (r // OWN) % nz, (r // (OWN * nz)) % nc

    def of_ring(r):
        return r % OWN, (r // (OWN * nc)) % nx, r // (OWN * na), (r // OWN) % nc

    def group(m, xi, zi, ci):
        return ((xi * nc + ci) * nz + zi) * OWN + m

    def ring(m, xi, zi, ci):
        return ((zi * nx + xi) * nc + ci) * OWN + m

    def a_copy(src, dst, send, recv, j):
        t = lax.rem(a + j, na)
        return pltpu.make_async_remote_copy(
            src_ref=src.at[t], dst_ref=dst.at[a], send_sem=send, recv_sem=recv,
            device_id={"x": t // nc, "c": lax.rem(t, nc)}, device_id_type=MESH_ID,
        )

    def z_copy(src, dst, send, recv, step):
        t = lax.rem(z + nz + step, nz)
        return pltpu.make_async_remote_copy(
            src_ref=src.at[t], dst_ref=dst.at[z], send_sem=send, recv_sem=recv,
            device_id={"z": t}, device_id_type=MESH_ID,
        )

    def all_a(src, dst, send, recv):
        def body(j, _):
            a_copy(src, dst, send, recv, j).start()
            return 0

        lax.fori_loop(1, na, body, 0)

    def ring_steps(most, least, *copy_args):
        def body(j, _):
            z_copy(*copy_args, most - j).start()
            z_copy(*copy_args, j - most).start()
            return 0

        lax.fori_loop(0, most - least + 1, body, 0)

    def ring_far(*copy_args):
        z_copy(*copy_args, nz // 2).start()
        if near + 1 < nz // 2:
            ring_steps(nz // 2 - 1, near + 1, *copy_args)

    def all_z(*copy_args):
        z_copy(*copy_args, nz // 2).start()
        ring_steps(nz // 2 - 1, 1, *copy_args)

    def all_a(src, dst, send, recv):
        def body(j, _):
            a_copy(src, dst, send, recv, j).start()
            return 0

        lax.fori_loop(1, na, body, 0)

    def ring_steps(most, least, *copy_args):
        def body(j, _):
            z_copy(*copy_args, most - j).start()
            z_copy(*copy_args, j - most).start()
            return 0

        lax.fori_loop(0, most - least + 1, body, 0)

    def ring_part(level, *copy_args):
        most = near * (level + 1)
        if most == nz // 2:
            z_copy(*copy_args, most).start()
            most -= 1
        if most > near * level:
            ring_steps(most, near * level + 1, *copy_args)

    def all_z(*copy_args):
        z_copy(*copy_args, nz // 2).start()
        ring_steps(nz // 2 - 1, 1, *copy_args)

    first, last = nz // 2 - nz // 8, nz // 2 + nz // 8

    def served_first(src, dst, send, recv):
        for j in range(last - first + 1):
            t = nz // 2 + ((j + 1) // 2) * (1 if j % 2 else -1)

            @pl.when(z != t)
            def _():
                z_copy(src, dst, send, recv, t - z).start()

    def served_later(*copy_args):
        def one(step):
            t = lax.rem(z + nz + step, nz)

            @pl.when(jnp.logical_or(t < first, t > last))
            def _():
                z_copy(*copy_args, step).start()

        def body(j, _):
            one(nz // 2 - 1 - j)
            one(j - nz // 2 + 1)
            return 0

        one(nz // 2)
        lax.fori_loop(0, nz // 2 - 1, body, 0)

    def arrived(name, ref, sem, n):
        part = ref.at[pl.ds(0, n)]
        with jax.named_scope(name):
            pltpu.make_async_copy(part, part, sem).wait()

    def by_group(perm, rows):
        return moved(perm[...], rows).reshape(na, OWN * nz, -1)

    def by_ring(perm, rows):
        return moved(perm[...], rows).reshape(nz, OWN * na, -1)

    def send_group(k):
        for copy in raw_copies(k):
            copy.wait()
        s1[k] = by_group(split_a, raw[k])
        all_a(s1.at[k], ar.at[k], a_send.at[k], a_recv.at[k])
        ar[k, a] = s1[k, a]

    def send_group(k):
        for copy in raw_copies(k):
            copy.wait()
        s1[k] = by_group(split_a, raw[k])
        all_a(s1.at[k], ar.at[k], a_send.at[k], a_recv.at[k])
        ar[k, a] = s1[k, a]

    def ring_args(k):
        return s2.at[k], zr.at[k], z_send.at[k], z_recv.at[k]

    def make_ring(k):
        for copy in raw_copies(k):
            copy.wait()
        s2[k] = by_ring(nat_z, raw[k])
        zr[k, z] = s2[k, z]

    nat_z[...] = one_hot(members, lambda r: natural(*of_ring(r)))
    make_ring(0)
    with jax.named_scope("greet"):
        pl.semaphore_wait(barrier, 2 * near + na - 1)
    signal_z(far, hop)
    signal_z(far, -hop)
    ring_steps(near, 1, *ring_args(0))
    for k in range(1, RING_FIRST):
        make_ring(k)
        ring_steps(near, 1, *ring_args(k))
    split_a[...] = one_hot(members, lambda r: natural(*of_group(r)))
    send_group(RING_FIRST)
    with jax.named_scope("far"):
        pl.semaphore_wait(far, 2)
    for k in range(RING_FIRST):
        ring_far(*ring_args(k))
    for k in range(RING_FIRST + 1, chunks):
        send_group(k)
    split_z[...] = one_hot(members, lambda r: group(*of_ring(r)))
    for k in range(RING_FIRST, chunks):
        arrived(f"a{k}", ar.at[k], a_recv.at[k], na - 1)
        rows = ar[k].reshape(members, CHUNK)
        if k < obs_chunks:
            s2[k] = by_ring(split_z, rows)
            all_z(*ring_args(k))
            zr[k, z] = s2[k, z]
        else:
            rows = moved(split_z[...], rows)
            for h in range(2):
                s2p[h] = rows[:, h * HALF : (h + 1) * HALF].reshape(nz, OWN * na, HALF)
                all_z(s2p.at[h], zrp.at[h], p_send.at[h], p_recv.at[h])
                zrp[h, z] = s2p[h, z]
    back_z[...] = one_hot(members, lambda r: ring(*of_group(r)))
    z_nat[...] = one_hot(members, lambda r: ring(*of_natural(r)))

    for k in range(RING_FIRST):
        arrived(f"z{k}", zr.at[k], z_recv.at[k], nz - 1)
        s1[k] = by_group(back_z, zr[k].reshape(members, CHUNK))
        all_a(s1.at[k], ar.at[k], a_send.at[k], a_recv.at[k])
        ar[k, a] = s1[k, a]

    for copy in row_copies:
        copy.wait()
    lines = lines_ref[0]
    eye = (
        lax.broadcasted_iota(jnp.int32, (members, members), 0)
        == lax.broadcasted_iota(jnp.int32, (members, members), 1)
    )
    gram[...] = jnp.where(eye, f32(members - 1), f32(0.0))
    pull[...] = jnp.zeros_like(pull)
    for k in (*range(RING_FIRST, obs_chunks - 1), *range(RING_FIRST), obs_chunks - 1):
        if k < RING_FIRST:
            arrived(f"a{k}", ar.at[k], a_recv.at[k], na - 1)
            values = jnp.dot(
                split_z[...], ar[k].reshape(members, CHUNK), preferred_element_type=f32
            )
        else:
            arrived(f"z{k}", zr.at[k], z_recv.at[k], nz - 1)
            values = zr[k].reshape(members, CHUNK).astype(f32)
        with jax.named_scope("gram"):
            deviat = values - jnp.mean(values, axis=0, keepdims=True)
            row_ids = k * CHUNK + lax.broadcasted_iota(jnp.int32, (1, CHUNK), 1)
            cols = pl.ds(k * CHUNK, CHUNK)
            weights = jnp.where(row_ids < lines, prec_ref[:, cols], f32(0.0))
            weighted = deviat * weights
            gram[...] += product(halves(weighted), halves(deviat), 1, 1)
            pull[...] += jnp.sum(weighted * dep_ref[:, cols], axis=1, keepdims=True)

    with jax.named_scope("newton"):
        system = gram[...]
        scale = jnp.sqrt(
            jnp.sum(jnp.sum(system * system, axis=1, keepdims=True), axis=0, keepdims=True)
        )
        identity = jnp.where(eye, f32(1.5), f32(0.0))
        iterate = system / scale
        root = identity - 0.5 * iterate
        factor_halves = halves(root)
        root_halves = factor_halves
        iterate_halves = halves(product(halves(iterate), factor_halves))
        for sweep in range(1, ITERS):
            factor_halves = halves(identity - 0.5 * product(root_halves, iterate_halves))
            root = product(factor_halves, root_halves)
            if sweep < ITERS - 1:
                iterate_halves = halves(product(iterate_halves, factor_halves))
                root_halves = halves(root)

        inner = jnp.sum(root * pull[...], axis=0, keepdims=True)
        shift = jnp.sum(root * inner, axis=1, keepdims=True) / scale
        shift = jnp.sum(jnp.where(eye, shift, f32(0.0)), axis=0, keepdims=True)
        transform = (math.sqrt(members - 1) / jnp.sqrt(scale)) * root + shift
        transform = halves(transform)
        kept = 1.0 - jnp.sum(
            transform[0].astype(f32) + transform[1].astype(f32), axis=1, keepdims=True
        )

    def result(h, rows, kept):
        arrived(f"p{h}", zrp.at[h], p_recv.at[h], nz - 1)
        quantities = zrp[h].reshape(members, HALF)
        center = jnp.mean(quantities.astype(f32), axis=0, keepdims=True)
        spread = jnp.dot(rows[0], quantities, preferred_element_type=f32) + (
            jnp.dot(rows[1], quantities, preferred_element_type=f32)
        )
        return (spread + kept * center).astype(bf16)

    for h in range(2):
        s5[h] = result(h, transform, kept).reshape(s5.shape[1:])

        def straight(step):
            t = lax.rem(z + nz + step, nz)
            for j in range(na):
                g = lax.rem(a + j, na)
                if j or not isinstance(step, int) or step:
                    pltpu.make_async_remote_copy(
                        src_ref=s5.at[h, t * na + g], dst_ref=db.at[h, z * na + a],
                        send_sem=db_send.at[h], recv_sem=db_recv.at[h],
                        device_id={"x": g // nc, "z": t, "c": lax.rem(g, nc)},
                        device_id_type=MESH_ID,
                    ).start()

        def straight_both(j, _):
            straight(nz // 2 - 1 - j)
            straight(j - nz // 2 + 1)
            return 0

        straight(nz // 2)
        lax.fori_loop(0, nz // 2 - 1, straight_both, 0)
        straight(0)
        db[h, z * na + a] = s5[h, z * na + a]
    for h in range(2):
        arrived(f"straight{h}", db.at[h], db_recv.at[h], na * nz - 1)
        rows = moved(z_nat[...], db[h].reshape(members, HALF))
        out_ref[:, :, h * HALF : (h + 1) * HALF] = rows.reshape(OWN, patches, HALF)
    for h in range(2):
        arrived("sent", s5.at[h], db_send.at[h], na * nz - 1)

    for k in range(chunks):
        arrived("sent", s1.at[k], a_send.at[k], na - 1)
        if k < obs_chunks:
            arrived("sent", s2.at[k], z_send.at[k], nz - 1)
    for half in range(2):
        arrived("sent", s2p.at[half], p_send.at[half], nz - 1)


def solution(mesh):
    nx, nz, nc = 4, 16, 2
    split = Mesh(mesh.devices.reshape(nx, nz, nc, mesh.shape["grp"]), ("x", "z", "c", "grp"))
    na = nx * nc
    members = OWN * na * nz

    def local(prior_members, mapped_prior, departure, precision_factor, measured_lines):
        chunks = mapped_prior.shape[2] // CHUNK + 1
        perm = pltpu.VMEM((members, members), bf16)
        by_a = (na, OWN * nz)
        by_z = (nz, OWN * na)
        dma = pltpu.SemaphoreType.DMA
        return pl.pallas_call(
            functools.partial(kernel, nx, nz, nc),
            out_shape=jax.ShapeDtypeStruct(prior_members.shape, bf16),
            in_specs=[
                pl.BlockSpec(memory_space=pltpu.HBM),
                pl.BlockSpec(memory_space=pltpu.HBM),
                pl.BlockSpec(memory_space=pltpu.HBM),
                pl.BlockSpec(memory_space=pltpu.HBM),
                pl.BlockSpec(memory_space=pltpu.SMEM),
            ],
            out_specs=pl.BlockSpec(memory_space=pltpu.VMEM),
            scratch_shapes=[
                pltpu.VMEM((chunks, members, CHUNK), bf16),
                pltpu.VMEM(departure.shape, f32),
                pltpu.VMEM(precision_factor.shape, f32),
                perm, perm, perm, perm, perm,
                pltpu.VMEM((chunks, *by_a, CHUNK), bf16),
                pltpu.VMEM((chunks, *by_a, CHUNK), bf16),
                pltpu.VMEM((chunks - 1, *by_z, CHUNK), bf16),
                pltpu.VMEM((chunks - 1, *by_z, CHUNK), bf16),
                pltpu.VMEM((2, *by_z, HALF), bf16),
                pltpu.VMEM((2, *by_z, HALF), bf16),
                pltpu.VMEM((2, na * nz, OWN, HALF), bf16),
                pltpu.VMEM((2, na * nz, OWN, HALF), bf16),
                pltpu.VMEM((members, members), f32),
                pltpu.VMEM((members, 1), f32),
                dma((chunks, OWN)),
                dma((2,)),
                pltpu.SemaphoreType.REGULAR,
                dma((chunks,)), dma((chunks,)),
                dma((chunks - 1,)), dma((chunks - 1,)),
                dma((2,)), dma((2,)),
                dma((2,)), dma((2,)),
            ],
            compiler_params=pltpu.CompilerParams(
                collective_id=0, has_side_effects=True, vmem_limit_bytes=48 << 20
            ),
        )(
            *(
                pltpu.with_memory_space_constraint(array, pltpu.HBM)
                for array in (
                    prior_members, mapped_prior, departure, precision_factor,
                )
            ),
            measured_lines,
        )

    return jax.shard_map(
        local,
        mesh=split,
        in_specs=(
            P(MEM, "grp", None),
            P(MEM, "grp", None),
            P(GRP_MEM, None),
            P(GRP_MEM, None),
            P(GRP_MEM),
        ),
        out_specs=P(MEM, "grp", None),
        check_vma=False,
    )
```

```python
import functools
import math

import jax
import jax.numpy as jnp
from jax import lax
from jax.experimental import pallas as pl
from jax.experimental.pallas import tpu as pltpu
from jax.sharding import Mesh
from jax.sharding import PartitionSpec as P

ITERS = 5
OWN = 2
CHUNK = 256
HALF = CHUNK
PIECES = CHUNK // HALF
RING_FIRST = 2
NEAR = 4
MEM = ("x", "z", "c")
GRP_MEM = ("grp", "x", "z", "c")
MESH_ID = pl.DeviceIdType.MESH

f32 = jnp.float32
bf16 = jnp.bfloat16


def one_hot(rows, source_of):
    out_row = lax.broadcasted_iota(jnp.int32, (rows, rows), 0)
    in_row = lax.broadcasted_iota(jnp.int32, (rows, rows), 1)
    return jnp.where(in_row == source_of(out_row), f32(1.0), f32(0.0)).astype(bf16)


def moved(perm, rows):
    return jnp.dot(perm, rows, preferred_element_type=f32).astype(bf16)


def halves(value):
    high = value.astype(bf16)
    return high, (value - high.astype(f32)).astype(bf16)


def product(left, right, contract=1, against=0):
    def dot(p, q):
        return lax.dot_general(
            p, q, (((contract,), (against,)), ((), ())), preferred_element_type=f32
        )

    return dot(left[0], right[0]) + (dot(left[0], right[1]) + dot(left[1], right[0]))


def kernel(
    nx, nz, nc,
    prior_hbm, mapped_hbm, dep_hbm, prec_hbm, lines_ref, out_ref,
    raw, dep_ref, prec_ref,
    split_a, split_z, back_z, nat_z, z_nat,
    s1, ar, s2, zr, s2p, zrp, s5, db, gram, pull,
    raw_sem, row_sem, far, a_send, a_recv, z_send, z_recv,
    p_send, p_recv, db_send, db_recv,
):
    na = nx * nc
    members = OWN * na * nz
    obs_chunks = mapped_hbm.shape[2] // CHUNK
    chunks = obs_chunks + 1
    patches = nx * nz * nc
    near = nz * NEAR // 16
    hop = nz // 2 - near
    x, z, c = lax.axis_index("x"), lax.axis_index("z"), lax.axis_index("c")
    a = x * nc + c

    barrier = pltpu.get_barrier_semaphore()

    def signal_z(sem, step):
        pl.semaphore_signal(
            sem, inc=1, device_id={"z": lax.rem(z + nz + step, nz)}, device_id_type=MESH_ID
        )

    def greet_a(j, _):
        t = lax.rem(a + j, na)
        pl.semaphore_signal(
            barrier, inc=1, device_id={"x": t // nc, "c": lax.rem(t, nc)}, device_id_type=MESH_ID
        )
        return 0

    def raw_copies(k):
        if k < obs_chunks:
            src = lambda m: mapped_hbm.at[m, :, pl.ds(k * CHUNK, CHUNK)]
        else:
            src = lambda m: prior_hbm.at[m]
        return [
            pltpu.make_async_copy(src(m), raw.at[k, pl.ds(m * patches, patches)], raw_sem.at[k, m])
            for m in range(OWN)
        ]

    row_copies = [
        pltpu.make_async_copy(dep_hbm, dep_ref, row_sem.at[0]),
        pltpu.make_async_copy(prec_hbm, prec_ref, row_sem.at[1]),
    ]
    for copy in raw_copies(0):
        copy.start()
    for step in range(near, 0, -1):
        signal_z(barrier, step)
        signal_z(barrier, -step)
    lax.fori_loop(1, na, greet_a, 0)
    for k in range(1, chunks):
        for copy in raw_copies(k):
            copy.start()
    for copy in row_copies:
        copy.start()

    def natural(m, xi, zi, ci):
        return m * patches + xi * (nz * nc) + zi * nc + ci

    def of_natural(r):
        return r // patches, (r // (nz * nc)) % nx, (r // nc) % nz, r % nc

    def of_group(r):
        return r % OWN, r // (OWN * nz * nc), (r // OWN) % nz, (r // (OWN * nz)) % nc

    def of_ring(r):
        return r % OWN, (r // (OWN * nc)) % nx, r // (OWN * na), (r // OWN) % nc

    def group(m, xi, zi, ci):
        return ((xi * nc + ci) * nz + zi) * OWN + m

    def ring(m, xi, zi, ci):
        return ((zi * nx + xi) * nc + ci) * OWN + m

    def a_copy(src, dst, send, recv, j):
        t = lax.rem(a + j, na)
        return pltpu.make_async_remote_copy(
            src_ref=src.at[t], dst_ref=dst.at[a], send_sem=send, recv_sem=recv,
            device_id={"x": t // nc, "c": lax.rem(t, nc)}, device_id_type=MESH_ID,
        )

    def z_copy(src, dst, send, recv, step):
        t = lax.rem(z + nz + step, nz)
        return pltpu.make_async_remote_copy(
            src_ref=src.at[t], dst_ref=dst.at[z], send_sem=send, recv_sem=recv,
            device_id={"z": t}, device_id_type=MESH_ID,
        )

    def all_a(src, dst, send, recv):
        def body(j, _):
            a_copy(src, dst, send, recv, j).start()
            return 0

        lax.fori_loop(1, na, body, 0)

    def ring_steps(most, least, *copy_args):
        def body(j, _):
            z_copy(*copy_args, most - j).start()
            z_copy(*copy_args, j - most).start()
            return 0

        lax.fori_loop(0, most - least + 1, body, 0)

    def ring_far(*copy_args):
        z_copy(*copy_args, nz // 2).start()
        if near + 1 < nz // 2:
            ring_steps(nz // 2 - 1, near + 1, *copy_args)

    def all_z(*copy_args):
        z_copy(*copy_args, nz // 2).start()
        ring_steps(nz // 2 - 1, 1, *copy_args)

    def all_a(src, dst, send, recv):
        def body(j, _):
            a_copy(src, dst, send, recv, j).start()
            return 0

        lax.fori_loop(1, na, body, 0)

    def ring_steps(most, least, *copy_args):
        def body(j, _):
            z_copy(*copy_args, most - j).start()
            z_copy(*copy_args, j - most).start()
            return 0

        lax.fori_loop(0, most - least + 1, body, 0)

    def ring_part(level, *copy_args):
        most = near * (level + 1)
        if most == nz // 2:
            z_copy(*copy_args, most).start()
            most -= 1
        if most > near * level:
            ring_steps(most, near * level + 1, *copy_args)

    def all_z(*copy_args):
        z_copy(*copy_args, nz // 2).start()
        ring_steps(nz // 2 - 1, 1, *copy_args)

    first, last = nz // 2 - nz // 8, nz // 2 + nz // 8

    def served_first(src, dst, send, recv):
        for j in range(last - first + 1):
            t = nz // 2 + ((j + 1) // 2) * (1 if j % 2 else -1)

            @pl.when(z != t)
            def _():
                z_copy(src, dst, send, recv, t - z).start()

    def served_later(*copy_args):
        def one(step):
            t = lax.rem(z + nz + step, nz)

            @pl.when(jnp.logical_or(t < first, t > last))
            def _():
                z_copy(*copy_args, step).start()

        def body(j, _):
            one(nz // 2 - 1 - j)
            one(j - nz // 2 + 1)
            return 0

        one(nz // 2)
        lax.fori_loop(0, nz // 2 - 1, body, 0)

    def arrived(name, ref, sem, n):
        part = ref.at[pl.ds(0, n)]
        with jax.named_scope(name):
            pltpu.make_async_copy(part, part, sem).wait()

    def by_group(perm, rows):
        return moved(perm[...], rows).reshape(na, OWN * nz, -1)

    def by_ring(perm, rows):
        return moved(perm[...], rows).reshape(nz, OWN * na, -1)

    def send_group(k):
        for copy in raw_copies(k):
            copy.wait()
        s1[k] = by_group(split_a, raw[k])
        all_a(s1.at[k], ar.at[k], a_send.at[k], a_recv.at[k])
        ar[k, a] = s1[k, a]

    def send_group(k):
        for copy in raw_copies(k):
            copy.wait()
        s1[k] = by_group(split_a, raw[k])
        all_a(s1.at[k], ar.at[k], a_send.at[k], a_recv.at[k])
        ar[k, a] = s1[k, a]

    def ring_args(k):
        return s2.at[k], zr.at[k], z_send.at[k], z_recv.at[k]

    def make_ring(k):
        for copy in raw_copies(k):
            copy.wait()
        s2[k] = by_ring(nat_z, raw[k])
        zr[k, z] = s2[k, z]

    nat_z[...] = one_hot(members, lambda r: natural(*of_ring(r)))
    make_ring(0)
    with jax.named_scope("greet"):
        pl.semaphore_wait(barrier, 2 * near + na - 1)
    signal_z(far, hop)
    signal_z(far, -hop)
    ring_steps(near, 1, *ring_args(0))
    for k in range(1, RING_FIRST):
        make_ring(k)
        ring_steps(near, 1, *ring_args(k))
    split_a[...] = one_hot(members, lambda r: natural(*of_group(r)))
    send_group(RING_FIRST)
    with jax.named_scope("far"):
        pl.semaphore_wait(far, 2)
    for k in range(RING_FIRST):
        ring_far(*ring_args(k))
    for k in range(RING_FIRST + 1, chunks):
        send_group(k)
    split_z[...] = one_hot(members, lambda r: group(*of_ring(r)))
    for k in range(RING_FIRST, chunks):
        arrived(f"a{k}", ar.at[k], a_recv.at[k], na - 1)
        rows = ar[k].reshape(members, CHUNK)
        if k < obs_chunks:
            s2[k] = by_ring(split_z, rows)
            all_z(*ring_args(k))
            zr[k, z] = s2[k, z]
        else:
            rows = moved(split_z[...], rows)
            for h in range(PIECES):
                s2p[h] = rows[:, h * HALF : (h + 1) * HALF].reshape(nz, OWN * na, HALF)
                all_z(s2p.at[h], zrp.at[h], p_send.at[h], p_recv.at[h])
                zrp[h, z] = s2p[h, z]
    back_z[...] = one_hot(members, lambda r: ring(*of_group(r)))
    z_nat[...] = one_hot(members, lambda r: ring(*of_natural(r)))

    for k in range(RING_FIRST):
        arrived(f"z{k}", zr.at[k], z_recv.at[k], nz - 1)
        s1[k] = by_group(back_z, zr[k].reshape(members, CHUNK))
        all_a(s1.at[k], ar.at[k], a_send.at[k], a_recv.at[k])
        ar[k, a] = s1[k, a]

    for copy in row_copies:
        copy.wait()
    lines = lines_ref[0]
    eye = (
        lax.broadcasted_iota(jnp.int32, (members, members), 0)
        == lax.broadcasted_iota(jnp.int32, (members, members), 1)
    )
    gram[...] = jnp.where(eye, f32(members - 1), f32(0.0))
    pull[...] = jnp.zeros_like(pull)
    for k in (*range(RING_FIRST, obs_chunks - 1), *range(RING_FIRST), obs_chunks - 1):
        if k < RING_FIRST:
            arrived(f"a{k}", ar.at[k], a_recv.at[k], na - 1)
            values = jnp.dot(
                split_z[...], ar[k].reshape(members, CHUNK), preferred_element_type=f32
            )
        else:
            arrived(f"z{k}", zr.at[k], z_recv.at[k], nz - 1)
            values = zr[k].reshape(members, CHUNK).astype(f32)
        with jax.named_scope("gram"):
            deviat = values - jnp.mean(values, axis=0, keepdims=True)
            row_ids = k * CHUNK + lax.broadcasted_iota(jnp.int32, (1, CHUNK), 1)
            cols = pl.ds(k * CHUNK, CHUNK)
            weights = jnp.where(row_ids < lines, prec_ref[:, cols], f32(0.0))
            weighted = deviat * weights
            gram[...] += product(halves(weighted), halves(deviat), 1, 1)
            pull[...] += jnp.sum(weighted * dep_ref[:, cols], axis=1, keepdims=True)

    with jax.named_scope("newton"):
        system = gram[...]
        scale = jnp.sqrt(
            jnp.sum(jnp.sum(system * system, axis=1, keepdims=True), axis=0, keepdims=True)
        )
        identity = jnp.where(eye, f32(1.5), f32(0.0))
        iterate = system / scale
        root = identity - 0.5 * iterate
        factor_halves = halves(root)
        root_halves = factor_halves
        iterate_halves = halves(product(halves(iterate), factor_halves))
        for sweep in range(1, ITERS):
            factor_halves = halves(identity - 0.5 * product(root_halves, iterate_halves))
            root = product(factor_halves, root_halves)
            if sweep < ITERS - 1:
                iterate_halves = halves(product(iterate_halves, factor_halves))
                root_halves = halves(root)

        inner = jnp.sum(root * pull[...], axis=0, keepdims=True)
        shift = jnp.sum(root * inner, axis=1, keepdims=True) / scale
        shift = jnp.sum(jnp.where(eye, shift, f32(0.0)), axis=0, keepdims=True)
        transform = (math.sqrt(members - 1) / jnp.sqrt(scale)) * root + shift
        kept = 1.0 - jnp.sum(transform, axis=1, keepdims=True)
        transform = halves(transform + kept / members)

    def result(h):
        arrived(f"p{h}", zrp.at[h], p_recv.at[h], nz - 1)
        quantities = zrp[h].reshape(members, HALF)
        return (
            jnp.dot(transform[0], quantities, preferred_element_type=f32)
            + jnp.dot(transform[1], quantities, preferred_element_type=f32)
        ).astype(bf16)

    for h in range(PIECES):
        s5[h] = result(h).reshape(s5.shape[1:])

        def straight(step):
            t = lax.rem(z + nz + step, nz)
            for j in range(na):
                g = lax.rem(a + j, na)
                if j or not isinstance(step, int) or step:
                    pltpu.make_async_remote_copy(
                        src_ref=s5.at[h, t * na + g], dst_ref=db.at[h, z * na + a],
                        send_sem=db_send.at[h], recv_sem=db_recv.at[h],
                        device_id={"x": g // nc, "z": t, "c": lax.rem(g, nc)},
                        device_id_type=MESH_ID,
                    ).start()

        def straight_both(j, _):
            straight(nz // 2 - 1 - j)
            straight(j - nz // 2 + 1)
            return 0

        straight(nz // 2)
        lax.fori_loop(0, nz // 2 - 1, straight_both, 0)
        straight(0)
        db[h, z * na + a] = s5[h, z * na + a]
    for h in range(PIECES):
        arrived(f"straight{h}", db.at[h], db_recv.at[h], na * nz - 1)
        rows = moved(z_nat[...], db[h].reshape(members, HALF))
        out_ref[:, :, h * HALF : (h + 1) * HALF] = rows.reshape(OWN, patches, HALF)
    for h in range(PIECES):
        arrived("sent", s5.at[h], db_send.at[h], na * nz - 1)

    for k in range(chunks):
        arrived("sent", s1.at[k], a_send.at[k], na - 1)
        if k < obs_chunks:
            arrived("sent", s2.at[k], z_send.at[k], nz - 1)
    for half in range(PIECES):
        arrived("sent", s2p.at[half], p_send.at[half], nz - 1)


def solution(mesh):
    nx, nz, nc = 4, 16, 2
    split = Mesh(mesh.devices.reshape(nx, nz, nc, mesh.shape["grp"]), ("x", "z", "c", "grp"))
    na = nx * nc
    members = OWN * na * nz

    def local(prior_members, mapped_prior, departure, precision_factor, measured_lines):
        chunks = mapped_prior.shape[2] // CHUNK + 1
        perm = pltpu.VMEM((members, members), bf16)
        by_a = (na, OWN * nz)
        by_z = (nz, OWN * na)
        dma = pltpu.SemaphoreType.DMA
        return pl.pallas_call(
            functools.partial(kernel, nx, nz, nc),
            out_shape=jax.ShapeDtypeStruct(prior_members.shape, bf16),
            in_specs=[
                pl.BlockSpec(memory_space=pltpu.HBM),
                pl.BlockSpec(memory_space=pltpu.HBM),
                pl.BlockSpec(memory_space=pltpu.HBM),
                pl.BlockSpec(memory_space=pltpu.HBM),
                pl.BlockSpec(memory_space=pltpu.SMEM),
            ],
            out_specs=pl.BlockSpec(memory_space=pltpu.VMEM),
            scratch_shapes=[
                pltpu.VMEM((chunks, members, CHUNK), bf16),
                pltpu.VMEM(departure.shape, f32),
                pltpu.VMEM(precision_factor.shape, f32),
                perm, perm, perm, perm, perm,
                pltpu.VMEM((chunks, *by_a, CHUNK), bf16),
                pltpu.VMEM((chunks, *by_a, CHUNK), bf16),
                pltpu.VMEM((chunks - 1, *by_z, CHUNK), bf16),
                pltpu.VMEM((chunks - 1, *by_z, CHUNK), bf16),
                pltpu.VMEM((PIECES, *by_z, HALF), bf16),
                pltpu.VMEM((PIECES, *by_z, HALF), bf16),
                pltpu.VMEM((PIECES, na * nz, OWN, HALF), bf16),
                pltpu.VMEM((PIECES, na * nz, OWN, HALF), bf16),
                pltpu.VMEM((members, members), f32),
                pltpu.VMEM((members, 1), f32),
                dma((chunks, OWN)),
                dma((2,)),
                pltpu.SemaphoreType.REGULAR,
                dma((chunks,)), dma((chunks,)),
                dma((chunks - 1,)), dma((chunks - 1,)),
                dma((2,)), dma((2,)),
                dma((2,)), dma((2,)),
            ],
            compiler_params=pltpu.CompilerParams(
                collective_id=0, has_side_effects=True, vmem_limit_bytes=48 << 20
            ),
        )(
            *(
                pltpu.with_memory_space_constraint(array, pltpu.HBM)
                for array in (
                    prior_members, mapped_prior, departure, precision_factor,
                )
            ),
            measured_lines,
        )

    return jax.shard_map(
        local,
        mesh=split,
        in_specs=(
            P(MEM, "grp", None),
            P(MEM, "grp", None),
            P(GRP_MEM, None),
            P(GRP_MEM, None),
            P(GRP_MEM),
        ),
        out_specs=P(MEM, "grp", None),
        check_vma=False,
    )
```

```python
import functools
import math

import jax
import jax.numpy as jnp
from jax import lax
from jax.experimental import pallas as pl
from jax.experimental.pallas import tpu as pltpu
from jax.sharding import Mesh
from jax.sharding import PartitionSpec as P

ITERS = 5
OWN = 2
CHUNK = 256
HALF = CHUNK
PIECES = CHUNK // HALF
RING_FIRST = 2
NEAR = 4
MEM = ("x", "z", "c")
GRP_MEM = ("grp", "x", "z", "c")
MESH_ID = pl.DeviceIdType.MESH

f32 = jnp.float32
bf16 = jnp.bfloat16


def one_hot(rows, source_of):
    out_row = lax.broadcasted_iota(jnp.int32, (rows, rows), 0)
    in_row = lax.broadcasted_iota(jnp.int32, (rows, rows), 1)
    return jnp.where(in_row == source_of(out_row), f32(1.0), f32(0.0)).astype(bf16)


def moved(perm, rows):
    return jnp.dot(perm, rows, preferred_element_type=f32).astype(bf16)


def halves(value):
    high = value.astype(bf16)
    return high, (value - high.astype(f32)).astype(bf16)


def product(left, right, contract=1, against=0):
    def dot(p, q):
        return lax.dot_general(
            p, q, (((contract,), (against,)), ((), ())), preferred_element_type=f32
        )

    return dot(left[0], right[0]) + (dot(left[0], right[1]) + dot(left[1], right[0]))


def kernel(
    nx, nz, nc,
    prior_hbm, mapped_hbm, dep_hbm, prec_hbm, lines_ref, out_ref,
    raw, dep_ref, prec_ref,
    split_a, split_z, back_z, nat_z, z_nat,
    s1, ar, s2, zr, s2p, zrp, s5, db, gram, pull,
    raw_sem, row_sem, far, a_send, a_recv, z_send, z_recv,
    p_send, p_recv, db_send, db_recv,
):
    na = nx * nc
    members = OWN * na * nz
    obs_chunks = mapped_hbm.shape[2] // CHUNK
    chunks = obs_chunks + 1
    patches = nx * nz * nc
    near = nz * NEAR // 16
    hop = nz // 2 - near
    x, z, c = lax.axis_index("x"), lax.axis_index("z"), lax.axis_index("c")
    a = x * nc + c

    barrier = pltpu.get_barrier_semaphore()

    def signal_z(sem, step):
        pl.semaphore_signal(
            sem, inc=1, device_id={"z": lax.rem(z + nz + step, nz)}, device_id_type=MESH_ID
        )

    def greet_a(j, _):
        t = lax.rem(a + j, na)
        pl.semaphore_signal(
            barrier, inc=1, device_id={"x": t // nc, "c": lax.rem(t, nc)}, device_id_type=MESH_ID
        )
        return 0

    def raw_copies(k):
        if k < obs_chunks:
            src = lambda m: mapped_hbm.at[m, :, pl.ds(k * CHUNK, CHUNK)]
        else:
            src = lambda m: prior_hbm.at[m]
        return [
            pltpu.make_async_copy(src(m), raw.at[k, pl.ds(m * patches, patches)], raw_sem.at[k])
            for m in range(OWN)
        ]

    row_copies = [
        pltpu.make_async_copy(dep_hbm, dep_ref, row_sem.at[0]),
        pltpu.make_async_copy(prec_hbm, prec_ref, row_sem.at[1]),
    ]
    for copy in raw_copies(0):
        copy.start()
    for step in range(near, 0, -1):
        signal_z(barrier, step)
        signal_z(barrier, -step)
    lax.fori_loop(1, na, greet_a, 0)
    for k in range(1, chunks):
        for copy in raw_copies(k):
            copy.start()
    for copy in row_copies:
        copy.start()

    def natural(m, xi, zi, ci):
        return m * patches + xi * (nz * nc) + zi * nc + ci

    def of_natural(r):
        return r // patches, (r // (nz * nc)) % nx, (r // nc) % nz, r % nc

    def of_group(r):
        return r % OWN, r // (OWN * nz * nc), (r // OWN) % nz, (r // (OWN * nz)) % nc

    def of_ring(r):
        return r % OWN, (r // (OWN * nc)) % nx, r // (OWN * na), (r // OWN) % nc

    def group(m, xi, zi, ci):
        return ((xi * nc + ci) * nz + zi) * OWN + m

    def ring(m, xi, zi, ci):
        return ((zi * nx + xi) * nc + ci) * OWN + m

    columns = [
        (lax.rem(x + dx, nx), lax.rem(c + dc, nc))
        for dx in sorted(range(nx), key=lambda d: -min(d, nx - d))
        for dc in range(nc - 1, -1, -1)
    ]

    def z_copy(src, dst, send, recv, step):
        t = lax.rem(z + nz + step, nz)
        return pltpu.make_async_remote_copy(
            src_ref=src.at[t], dst_ref=dst.at[z], send_sem=send, recv_sem=recv,
            device_id={"z": t}, device_id_type=MESH_ID,
        )

    def all_a(src, dst, send, recv):
        for to_x, to_c in columns[:-1]:
            pltpu.make_async_remote_copy(
                src_ref=src.at[to_x * nc + to_c], dst_ref=dst.at[a], send_sem=send, recv_sem=recv,
                device_id={"x": to_x, "c": to_c}, device_id_type=MESH_ID,
            ).start()

    def ring_steps(most, least, *copy_args):
        def body(j, _):
            z_copy(*copy_args, most - j).start()
            z_copy(*copy_args, j - most).start()
            return 0

        lax.fori_loop(0, most - least + 1, body, 0)

    def ring_far(*copy_args):
        z_copy(*copy_args, nz // 2).start()
        if near + 1 < nz // 2:
            ring_steps(nz // 2 - 1, near + 1, *copy_args)

    def all_z(*copy_args):
        z_copy(*copy_args, nz // 2).start()
        ring_steps(nz // 2 - 1, 1, *copy_args)

    def arrived(name, ref, sem, n):
        part = ref.at[pl.ds(0, n)]
        with jax.named_scope(name):
            pltpu.make_async_copy(part, part, sem).wait()

    def by_group(perm, rows):
        return moved(perm[...], rows).reshape(na, OWN * nz, -1)

    def by_ring(perm, rows):
        return moved(perm[...], rows).reshape(nz, OWN * na, -1)

    def send_group(k):
        pltpu.make_async_copy(raw.at[k], raw.at[k], raw_sem.at[k]).wait()
        s1[k] = by_group(split_a, raw[k])
        all_a(s1.at[k], ar.at[k], a_send, a_recv.at[k])
        ar[k, a] = s1[k, a]

    def ring_args(k):
        return s2.at[k], zr.at[k], z_send, z_recv.at[k]

    def make_ring(k):
        pltpu.make_async_copy(raw.at[k], raw.at[k], raw_sem.at[k]).wait()
        s2[k] = by_ring(nat_z, raw[k])
        zr[k, z] = s2[k, z]

    nat_z[...] = one_hot(members, lambda r: natural(*of_ring(r)))
    make_ring(0)
    with jax.named_scope("greet"):
        pl.semaphore_wait(barrier, 2 * near + na - 1)
    signal_z(far, hop)
    signal_z(far, -hop)
    ring_steps(near, 1, *ring_args(0))
    for k in range(1, RING_FIRST):
        make_ring(k)
        ring_steps(near, 1, *ring_args(k))
    split_a[...] = one_hot(members, lambda r: natural(*of_group(r)))
    send_group(RING_FIRST)
    with jax.named_scope("far"):
        pl.semaphore_wait(far, 2)
    for k in range(RING_FIRST):
        ring_far(*ring_args(k))
    for k in range(RING_FIRST + 1, chunks):
        send_group(k)
    split_z[...] = one_hot(members, lambda r: group(*of_ring(r)))
    for k in range(RING_FIRST, chunks):
        arrived(f"a{k}", ar.at[k], a_recv.at[k], na - 1)
        rows = ar[k].reshape(members, CHUNK)
        if k < obs_chunks:
            s2[k] = by_ring(split_z, rows)
            all_z(*ring_args(k))
            zr[k, z] = s2[k, z]
        else:
            rows = moved(split_z[...], rows)
            for h in range(PIECES):
                s2p[h] = rows[:, h * HALF : (h + 1) * HALF].reshape(nz, OWN * na, HALF)
                all_z(s2p.at[h], zrp.at[h], p_send.at[h], p_recv.at[h])
                zrp[h, z] = s2p[h, z]
    back_z[...] = one_hot(members, lambda r: ring(*of_group(r)))
    z_nat[...] = one_hot(members, lambda r: ring(*of_natural(r)))

    for k in range(RING_FIRST):
        arrived(f"z{k}", zr.at[k], z_recv.at[k], nz - 1)
        s1[k] = by_group(back_z, zr[k].reshape(members, CHUNK))
        all_a(s1.at[k], ar.at[k], a_send, a_recv.at[k])
        ar[k, a] = s1[k, a]

    for copy in row_copies:
        copy.wait()
    lines = lines_ref[0]
    eye = (
        lax.broadcasted_iota(jnp.int32, (members, members), 0)
        == lax.broadcasted_iota(jnp.int32, (members, members), 1)
    )
    gram[...] = jnp.where(eye, f32(members - 1), f32(0.0))
    pull[...] = jnp.zeros_like(pull)
    for k in (*range(RING_FIRST, obs_chunks - 1), *range(RING_FIRST), obs_chunks - 1):
        if k < RING_FIRST:
            arrived(f"a{k}", ar.at[k], a_recv.at[k], na - 1)
            values = jnp.dot(
                split_z[...], ar[k].reshape(members, CHUNK), preferred_element_type=f32
            )
        else:
            arrived(f"z{k}", zr.at[k], z_recv.at[k], nz - 1)
            values = zr[k].reshape(members, CHUNK).astype(f32)
        with jax.named_scope("gram"):
            deviat = values - jnp.mean(values, axis=0, keepdims=True)
            row_ids = k * CHUNK + lax.broadcasted_iota(jnp.int32, (1, CHUNK), 1)
            cols = pl.ds(k * CHUNK, CHUNK)
            weights = jnp.where(row_ids < lines, prec_ref[:, cols], f32(0.0))
            weighted = deviat * weights
            gram[...] += product(halves(weighted), halves(deviat), 1, 1)
            pull[...] += jnp.sum(weighted * dep_ref[:, cols], axis=1, keepdims=True)

    with jax.named_scope("newton"):
        system = gram[...]
        scale = jnp.sqrt(
            jnp.sum(jnp.sum(system * system, axis=1, keepdims=True), axis=0, keepdims=True)
        )
        identity = jnp.where(eye, f32(1.5), f32(0.0))
        iterate = system / scale
        root = identity - 0.5 * iterate
        factor_halves = halves(root)
        root_halves = factor_halves
        iterate_halves = halves(product(halves(iterate), factor_halves))
        for sweep in range(1, ITERS):
            factor_halves = halves(identity - 0.5 * product(root_halves, iterate_halves))
            root = product(factor_halves, root_halves)
            if sweep < ITERS - 1:
                iterate_halves = halves(product(iterate_halves, factor_halves))
                root_halves = halves(root)

        inner = jnp.sum(root * pull[...], axis=0, keepdims=True)
        shift = jnp.sum(root * inner, axis=1, keepdims=True) / scale
        shift = jnp.sum(jnp.where(eye, shift, f32(0.0)), axis=0, keepdims=True)
        transform = (math.sqrt(members - 1) / jnp.sqrt(scale)) * root + shift
        kept = 1.0 - jnp.sum(transform, axis=1, keepdims=True)
        transform = halves(transform + kept / members)

    def result(h):
        arrived(f"p{h}", zrp.at[h], p_recv.at[h], nz - 1)
        quantities = zrp[h].reshape(members, HALF)
        return (
            jnp.dot(transform[0], quantities, preferred_element_type=f32)
            + jnp.dot(transform[1], quantities, preferred_element_type=f32)
        ).astype(bf16)

    for h in range(PIECES):
        s5[h] = result(h).reshape(s5.shape[1:])

        def straight(step):
            t = lax.rem(z + nz + step, nz)
            own = isinstance(step, int) and step == 0
            for to_x, to_c in columns[:-1] if own else columns:
                pltpu.make_async_remote_copy(
                    src_ref=s5.at[h, (t * nx + to_x) * nc + to_c], dst_ref=db.at[h, z * na + a],
                    send_sem=db_send.at[h], recv_sem=db_recv.at[h],
                    device_id={"x": to_x, "z": t, "c": to_c}, device_id_type=MESH_ID,
                ).start()

        def straight_both(j, _):
            straight(nz // 2 - 1 - j)
            straight(j - nz // 2 + 1)
            return 0

        straight(nz // 2)
        lax.fori_loop(0, nz // 2 - 1, straight_both, 0)
        straight(0)
        db[h, z * na + a] = s5[h, z * na + a]
    for h in range(PIECES):
        arrived(f"straight{h}", db.at[h], db_recv.at[h], na * nz - 1)
        rows = moved(z_nat[...], db[h].reshape(members, HALF))
        out_ref[:, :, h * HALF : (h + 1) * HALF] = rows.reshape(OWN, patches, HALF)
    for h in range(PIECES):
        arrived("sent", s5.at[h], db_send.at[h], na * nz - 1)

    for part, sem in (
        (s1.at[:, pl.ds(0, na - 1)], a_send), (s2.at[:, pl.ds(0, nz - 1)], z_send)
    ):
        pltpu.make_async_copy(part, part, sem).wait()
    for half in range(PIECES):
        arrived("sent", s2p.at[half], p_send.at[half], nz - 1)


def solution(mesh):
    nx, nz, nc = 4, 16, 2
    split = Mesh(mesh.devices.reshape(nx, nz, nc, mesh.shape["grp"]), ("x", "z", "c", "grp"))
    na = nx * nc
    members = OWN * na * nz

    def local(prior_members, mapped_prior, departure, precision_factor, measured_lines):
        chunks = mapped_prior.shape[2] // CHUNK + 1
        perm = pltpu.VMEM((members, members), bf16)
        by_a = (na, OWN * nz)
        by_z = (nz, OWN * na)
        dma = pltpu.SemaphoreType.DMA
        return pl.pallas_call(
            functools.partial(kernel, nx, nz, nc),
            out_shape=jax.ShapeDtypeStruct(prior_members.shape, bf16),
            in_specs=[
                pl.BlockSpec(memory_space=pltpu.HBM),
                pl.BlockSpec(memory_space=pltpu.HBM),
                pl.BlockSpec(memory_space=pltpu.HBM),
                pl.BlockSpec(memory_space=pltpu.HBM),
                pl.BlockSpec(memory_space=pltpu.SMEM),
            ],
            out_specs=pl.BlockSpec(memory_space=pltpu.VMEM),
            scratch_shapes=[
                pltpu.VMEM((chunks, members, CHUNK), bf16),
                pltpu.VMEM(departure.shape, f32),
                pltpu.VMEM(precision_factor.shape, f32),
                perm, perm, perm, perm, perm,
                pltpu.VMEM((chunks, *by_a, CHUNK), bf16),
                pltpu.VMEM((chunks, *by_a, CHUNK), bf16),
                pltpu.VMEM((chunks - 1, *by_z, CHUNK), bf16),
                pltpu.VMEM((chunks - 1, *by_z, CHUNK), bf16),
                pltpu.VMEM((PIECES, *by_z, HALF), bf16),
                pltpu.VMEM((PIECES, *by_z, HALF), bf16),
                pltpu.VMEM((PIECES, na * nz, OWN, HALF), bf16),
                pltpu.VMEM((PIECES, na * nz, OWN, HALF), bf16),
                pltpu.VMEM((members, members), f32),
                pltpu.VMEM((members, 1), f32),
                dma((chunks,)),
                dma((2,)),
                pltpu.SemaphoreType.REGULAR,
                dma, dma((chunks,)),
                dma, dma((chunks - 1,)),
                dma((PIECES,)), dma((PIECES,)),
                dma((PIECES,)), dma((PIECES,)),
            ],
            compiler_params=pltpu.CompilerParams(
                collective_id=0, has_side_effects=True, vmem_limit_bytes=48 << 20
            ),
        )(
            *(
                pltpu.with_memory_space_constraint(array, pltpu.HBM)
                for array in (
                    prior_members, mapped_prior, departure, precision_factor,
                )
            ),
            measured_lines,
        )

    return jax.shard_map(
        local,
        mesh=split,
        in_specs=(
            P(MEM, "grp", None),
            P(MEM, "grp", None),
            P(GRP_MEM, None),
            P(GRP_MEM, None),
            P(GRP_MEM),
        ),
        out_specs=P(MEM, "grp", None),
        check_vma=False,
    )
```

```python
import functools
import math

import jax
import jax.numpy as jnp
from jax import lax
from jax.experimental import pallas as pl
from jax.experimental.pallas import tpu as pltpu
from jax.sharding import Mesh
from jax.sharding import PartitionSpec as P

ITERS = 5
OWN = 2
CHUNK = 256
HALF = CHUNK
PIECES = CHUNK // HALF
RING_FIRST = 2
NEAR = 4
MEM = ("x", "z", "c")
GRP_MEM = ("grp", "x", "z", "c")
MESH_ID = pl.DeviceIdType.MESH

f32 = jnp.float32
bf16 = jnp.bfloat16


def one_hot(rows, source_of):
    out_row = lax.broadcasted_iota(jnp.int32, (rows, rows), 0)
    in_row = lax.broadcasted_iota(jnp.int32, (rows, rows), 1)
    return jnp.where(in_row == source_of(out_row), f32(1.0), f32(0.0)).astype(bf16)


def moved(perm, rows):
    return jnp.dot(perm, rows, preferred_element_type=f32).astype(bf16)


def halves(value):
    high = value.astype(bf16)
    return high, (value - high.astype(f32)).astype(bf16)


def product(left, right, contract=1, against=0):
    def dot(p, q):
        return lax.dot_general(
            p, q, (((contract,), (against,)), ((), ())), preferred_element_type=f32
        )

    return dot(left[0], right[0]) + (dot(left[0], right[1]) + dot(left[1], right[0]))


def kernel(
    nx, nz, nc,
    prior_hbm, mapped_hbm, dep_hbm, prec_hbm, lines_ref, out_ref,
    raw, dep_ref, prec_ref,
    split_a, split_z, back_z, nat_z, z_nat,
    s1, ar, s2, zr, s2p, zrp, s5, db, gram, pull,
    raw_sem, row_sem, far, a_send, a_recv, z_send, z_recv,
    p_send, p_recv, db_send, db_recv,
):
    na = nx * nc
    members = OWN * na * nz
    obs_chunks = mapped_hbm.shape[2] // CHUNK
    chunks = obs_chunks + 1
    patches = nx * nz * nc
    near = nz * NEAR // 16
    hop = nz // 2 - near
    x, z, c = lax.axis_index("x"), lax.axis_index("z"), lax.axis_index("c")
    a = x * nc + c

    barrier = pltpu.get_barrier_semaphore()

    def signal_z(sem, step):
        pl.semaphore_signal(
            sem, inc=1, device_id={"z": lax.rem(z + nz + step, nz)}, device_id_type=MESH_ID
        )

    def greet_a(j, _):
        t = lax.rem(a + j, na)
        pl.semaphore_signal(
            barrier, inc=1, device_id={"x": t // nc, "c": lax.rem(t, nc)}, device_id_type=MESH_ID
        )
        return 0

    def raw_copies(k):
        if k < obs_chunks:
            src = lambda m: mapped_hbm.at[m, :, pl.ds(k * CHUNK, CHUNK)]
        else:
            src = lambda m: prior_hbm.at[m]
        return [
            pltpu.make_async_copy(src(m), raw.at[k, pl.ds(m * patches, patches)], raw_sem.at[k])
            for m in range(OWN)
        ]

    row_copies = [
        pltpu.make_async_copy(dep_hbm, dep_ref, row_sem.at[0]),
        pltpu.make_async_copy(prec_hbm, prec_ref, row_sem.at[1]),
    ]
    for copy in raw_copies(0):
        copy.start()
    for step in range(near, 0, -1):
        signal_z(barrier, step)
        signal_z(barrier, -step)
    lax.fori_loop(1, na, greet_a, 0)
    for k in range(1, chunks):
        for copy in raw_copies(k):
            copy.start()
    for copy in row_copies:
        copy.start()

    def natural(m, xi, zi, ci):
        return m * patches + xi * (nz * nc) + zi * nc + ci

    def of_natural(r):
        return r // patches, (r // (nz * nc)) % nx, (r // nc) % nz, r % nc

    def of_group(r):
        return r % OWN, r // (OWN * nz * nc), (r // OWN) % nz, (r // (OWN * nz)) % nc

    def of_ring(r):
        return r % OWN, (r // (OWN * nc)) % nx, r // (OWN * na), (r // OWN) % nc

    def group(m, xi, zi, ci):
        return ((xi * nc + ci) * nz + zi) * OWN + m

    def ring(m, xi, zi, ci):
        return ((zi * nx + xi) * nc + ci) * OWN + m

    columns = [
        (lax.rem(x + dx, nx), lax.rem(c + dc, nc))
        for dx in sorted(range(nx), key=lambda d: -min(d, nx - d))
        for dc in range(nc - 1, -1, -1)
    ]

    def z_copy(src, dst, send, recv, step):
        t = lax.rem(z + nz + step, nz)
        return pltpu.make_async_remote_copy(
            src_ref=src.at[t], dst_ref=dst.at[z], send_sem=send, recv_sem=recv,
            device_id={"z": t}, device_id_type=MESH_ID,
        )

    def all_a(src, dst, send, recv):
        for to_x, to_c in columns[:-1]:
            pltpu.make_async_remote_copy(
                src_ref=src.at[to_x * nc + to_c], dst_ref=dst.at[a], send_sem=send, recv_sem=recv,
                device_id={"x": to_x, "c": to_c}, device_id_type=MESH_ID,
            ).start()

    def ring_steps(most, least, *copy_args):
        def body(j, _):
            z_copy(*copy_args, most - j).start()
            z_copy(*copy_args, j - most).start()
            return 0

        lax.fori_loop(0, most - least + 1, body, 0, unroll=True)

    def ring_far(*copy_args):
        z_copy(*copy_args, nz // 2).start()
        if near + 1 < nz // 2:
            ring_steps(nz // 2 - 1, near + 1, *copy_args)

    def all_z(*copy_args):
        z_copy(*copy_args, nz // 2).start()
        ring_steps(nz // 2 - 1, 1, *copy_args)

    def arrived(name, ref, sem, n):
        part = ref.at[pl.ds(0, n)]
        with jax.named_scope(name):
            pltpu.make_async_copy(part, part, sem).wait()

    def by_group(perm, rows):
        return moved(perm[...], rows).reshape(na, OWN * nz, -1)

    def by_ring(perm, rows):
        return moved(perm[...], rows).reshape(nz, OWN * na, -1)

    def send_group(k):
        pltpu.make_async_copy(raw.at[k], raw.at[k], raw_sem.at[k]).wait()
        s1[k] = by_group(split_a, raw[k])
        all_a(s1.at[k], ar.at[k], a_send, a_recv.at[k])
        ar[k, a] = s1[k, a]

    def ring_args(k):
        return s2.at[k], zr.at[k], z_send, z_recv.at[k]

    def make_ring(k):
        pltpu.make_async_copy(raw.at[k], raw.at[k], raw_sem.at[k]).wait()
        s2[k] = by_ring(nat_z, raw[k])
        zr[k, z] = s2[k, z]

    nat_z[...] = one_hot(members, lambda r: natural(*of_ring(r)))
    make_ring(0)
    with jax.named_scope("greet"):
        pl.semaphore_wait(barrier, 2 * near + na - 1)
    signal_z(far, hop)
    signal_z(far, -hop)
    ring_steps(near, 1, *ring_args(0))
    for k in range(1, RING_FIRST):
        make_ring(k)
        ring_steps(near, 1, *ring_args(k))
    split_a[...] = one_hot(members, lambda r: natural(*of_group(r)))
    send_group(RING_FIRST)
    with jax.named_scope("far"):
        pl.semaphore_wait(far, 2)
    for k in range(RING_FIRST):
        ring_far(*ring_args(k))
    for k in range(RING_FIRST + 1, chunks):
        send_group(k)
    split_z[...] = one_hot(members, lambda r: group(*of_ring(r)))
    for k in range(RING_FIRST, chunks):
        arrived(f"a{k}", ar.at[k], a_recv.at[k], na - 1)
        rows = ar[k].reshape(members, CHUNK)
        if k < obs_chunks:
            s2[k] = by_ring(split_z, rows)
            all_z(*ring_args(k))
            zr[k, z] = s2[k, z]
        else:
            rows = moved(split_z[...], rows)
            for h in range(PIECES):
                s2p[h] = rows[:, h * HALF : (h + 1) * HALF].reshape(nz, OWN * na, HALF)
                all_z(s2p.at[h], zrp.at[h], p_send.at[h], p_recv.at[h])
                zrp[h, z] = s2p[h, z]
    back_z[...] = one_hot(members, lambda r: ring(*of_group(r)))
    z_nat[...] = one_hot(members, lambda r: ring(*of_natural(r)))

    for k in range(RING_FIRST):
        arrived(f"z{k}", zr.at[k], z_recv.at[k], nz - 1)
        s1[k] = by_group(back_z, zr[k].reshape(members, CHUNK))
        all_a(s1.at[k], ar.at[k], a_send, a_recv.at[k])
        ar[k, a] = s1[k, a]

    for copy in row_copies:
        copy.wait()
    lines = lines_ref[0]
    eye = (
        lax.broadcasted_iota(jnp.int32, (members, members), 0)
        == lax.broadcasted_iota(jnp.int32, (members, members), 1)
    )
    gram[...] = jnp.where(eye, f32(members - 1), f32(0.0))
    pull[...] = jnp.zeros_like(pull)
    for k in (*range(RING_FIRST, obs_chunks - 1), *range(RING_FIRST), obs_chunks - 1):
        if k < RING_FIRST:
            arrived(f"a{k}", ar.at[k], a_recv.at[k], na - 1)
            values = jnp.dot(
                split_z[...], ar[k].reshape(members, CHUNK), preferred_element_type=f32
            )
        else:
            arrived(f"z{k}", zr.at[k], z_recv.at[k], nz - 1)
            values = zr[k].reshape(members, CHUNK).astype(f32)
        with jax.named_scope("gram"):
            deviat = values - jnp.mean(values, axis=0, keepdims=True)
            row_ids = k * CHUNK + lax.broadcasted_iota(jnp.int32, (1, CHUNK), 1)
            cols = pl.ds(k * CHUNK, CHUNK)
            weights = jnp.where(row_ids < lines, prec_ref[:, cols], f32(0.0))
            weighted = deviat * weights
            gram[...] += product(halves(weighted), halves(deviat), 1, 1)
            pull[...] += jnp.sum(weighted * dep_ref[:, cols], axis=1, keepdims=True)

    with jax.named_scope("newton"):
        system = gram[...]
        scale = jnp.sqrt(
            jnp.sum(jnp.sum(system * system, axis=1, keepdims=True), axis=0, keepdims=True)
        )
        identity = jnp.where(eye, f32(1.5), f32(0.0))
        iterate = system / scale
        root = identity - 0.5 * iterate
        factor_halves = halves(root)
        root_halves = factor_halves
        iterate_halves = halves(product(halves(iterate), factor_halves))
        for sweep in range(1, ITERS):
            factor_halves = halves(identity - 0.5 * product(root_halves, iterate_halves))
            root = product(factor_halves, root_halves)
            if sweep < ITERS - 1:
                iterate_halves = halves(product(iterate_halves, factor_halves))
                root_halves = halves(root)

        inner = jnp.sum(root * pull[...], axis=0, keepdims=True)
        shift = jnp.sum(root * inner, axis=1, keepdims=True) / scale
        shift = jnp.sum(jnp.where(eye, shift, f32(0.0)), axis=0, keepdims=True)
        transform = (math.sqrt(members - 1) / jnp.sqrt(scale)) * root + shift
        kept = 1.0 - jnp.sum(transform, axis=1, keepdims=True)
        transform = halves(transform + kept / members)

    def result(h):
        arrived(f"p{h}", zrp.at[h], p_recv.at[h], nz - 1)
        quantities = zrp[h].reshape(members, HALF)
        return (
            jnp.dot(transform[0], quantities, preferred_element_type=f32)
            + jnp.dot(transform[1], quantities, preferred_element_type=f32)
        ).astype(bf16)

    for h in range(PIECES):
        s5[h] = result(h).reshape(s5.shape[1:])

        def straight(step):
            t = lax.rem(z + nz + step, nz)
            own = isinstance(step, int) and step == 0
            for to_x, to_c in columns[:-1] if own else columns:
                pltpu.make_async_remote_copy(
                    src_ref=s5.at[h, (t * nx + to_x) * nc + to_c], dst_ref=db.at[h, z * na + a],
                    send_sem=db_send.at[h], recv_sem=db_recv.at[h],
                    device_id={"x": to_x, "z": t, "c": to_c}, device_id_type=MESH_ID,
                ).start()

        def straight_both(j, _):
            straight(nz // 2 - 1 - j)
            straight(j - nz // 2 + 1)
            return 0

        straight(nz // 2)
        lax.fori_loop(0, nz // 2 - 1, straight_both, 0, unroll=True)
        straight(0)
        db[h, z * na + a] = s5[h, z * na + a]
    for h in range(PIECES):
        arrived(f"straight{h}", db.at[h], db_recv.at[h], na * nz - 1)
        rows = moved(z_nat[...], db[h].reshape(members, HALF))
        out_ref[:, :, h * HALF : (h + 1) * HALF] = rows.reshape(OWN, patches, HALF)
    for h in range(PIECES):
        arrived("sent", s5.at[h], db_send.at[h], na * nz - 1)

    for part, sem in (
        (s1.at[:, pl.ds(0, na - 1)], a_send), (s2.at[:, pl.ds(0, nz - 1)], z_send)
    ):
        pltpu.make_async_copy(part, part, sem).wait()
    for half in range(PIECES):
        arrived("sent", s2p.at[half], p_send.at[half], nz - 1)


def solution(mesh):
    nx, nz, nc = 4, 16, 2
    split = Mesh(mesh.devices.reshape(nx, nz, nc, mesh.shape["grp"]), ("x", "z", "c", "grp"))
    na = nx * nc
    members = OWN * na * nz

    def local(prior_members, mapped_prior, departure, precision_factor, measured_lines):
        chunks = mapped_prior.shape[2] // CHUNK + 1
        perm = pltpu.VMEM((members, members), bf16)
        by_a = (na, OWN * nz)
        by_z = (nz, OWN * na)
        dma = pltpu.SemaphoreType.DMA
        return pl.pallas_call(
            functools.partial(kernel, nx, nz, nc),
            out_shape=jax.ShapeDtypeStruct(prior_members.shape, bf16),
            in_specs=[
                pl.BlockSpec(memory_space=pltpu.HBM),
                pl.BlockSpec(memory_space=pltpu.HBM),
                pl.BlockSpec(memory_space=pltpu.HBM),
                pl.BlockSpec(memory_space=pltpu.HBM),
                pl.BlockSpec(memory_space=pltpu.SMEM),
            ],
            out_specs=pl.BlockSpec(memory_space=pltpu.VMEM),
            scratch_shapes=[
                pltpu.VMEM((chunks, members, CHUNK), bf16),
                pltpu.VMEM(departure.shape, f32),
                pltpu.VMEM(precision_factor.shape, f32),
                perm, perm, perm, perm, perm,
                pltpu.VMEM((chunks, *by_a, CHUNK), bf16),
                pltpu.VMEM((chunks, *by_a, CHUNK), bf16),
                pltpu.VMEM((chunks - 1, *by_z, CHUNK), bf16),
                pltpu.VMEM((chunks - 1, *by_z, CHUNK), bf16),
                pltpu.VMEM((PIECES, *by_z, HALF), bf16),
                pltpu.VMEM((PIECES, *by_z, HALF), bf16),
                pltpu.VMEM((PIECES, na * nz, OWN, HALF), bf16),
                pltpu.VMEM((PIECES, na * nz, OWN, HALF), bf16),
                pltpu.VMEM((members, members), f32),
                pltpu.VMEM((members, 1), f32),
                dma((chunks,)),
                dma((2,)),
                pltpu.SemaphoreType.REGULAR,
                dma, dma((chunks,)),
                dma, dma((chunks - 1,)),
                dma((PIECES,)), dma((PIECES,)),
                dma((PIECES,)), dma((PIECES,)),
            ],
            compiler_params=pltpu.CompilerParams(
                collective_id=0, has_side_effects=True, vmem_limit_bytes=48 << 20
            ),
        )(
            *(
                pltpu.with_memory_space_constraint(array, pltpu.HBM)
                for array in (
                    prior_members, mapped_prior, departure, precision_factor,
                )
            ),
            measured_lines,
        )

    return jax.shard_map(
        local,
        mesh=split,
        in_specs=(
            P(MEM, "grp", None),
            P(MEM, "grp", None),
            P(GRP_MEM, None),
            P(GRP_MEM, None),
            P(GRP_MEM),
        ),
        out_specs=P(MEM, "grp", None),
        check_vma=False,
    )
```

```python
import functools
import math

import jax
import jax.numpy as jnp
from jax import lax
from jax.experimental import pallas as pl
from jax.experimental.pallas import tpu as pltpu
from jax.sharding import Mesh
from jax.sharding import PartitionSpec as P

ITERS = 5
OWN = 2
CHUNK = 256
HALF = CHUNK
PIECES = CHUNK // HALF
RING_FIRST = 2
NEAR = 4
MEM = ("x", "z", "c")
GRP_MEM = ("grp", "x", "z", "c")
MESH_ID = pl.DeviceIdType.MESH

f32 = jnp.float32
bf16 = jnp.bfloat16


def one_hot(rows, source_of):
    out_row = lax.broadcasted_iota(jnp.int32, (rows, rows), 0)
    in_row = lax.broadcasted_iota(jnp.int32, (rows, rows), 1)
    return jnp.where(in_row == source_of(out_row), f32(1.0), f32(0.0)).astype(bf16)


def moved(perm, rows):
    return jnp.dot(perm, rows, preferred_element_type=f32).astype(bf16)


def halves(value):
    high = value.astype(bf16)
    return high, (value - high.astype(f32)).astype(bf16)


def product(left, right, contract=1, against=0):
    def dot(p, q):
        return lax.dot_general(
            p, q, (((contract,), (against,)), ((), ())), preferred_element_type=f32
        )

    return dot(left[0], right[0]) + (dot(left[0], right[1]) + dot(left[1], right[0]))


def kernel(
    nx, nz, nc,
    prior_hbm, mapped_hbm, dep_hbm, prec_hbm, lines_ref, out_ref,
    raw, dep_ref, prec_ref,
    split_a, split_z, back_z, nat_z, z_nat,
    s1, ar, s2, zr, s2p, zrp, s5, db, gram, pull,
    raw_sem, row_sem, far, a_send, a_recv, z_send, z_recv,
    p_send, p_recv, db_send, db_recv,
):
    na = nx * nc
    members = OWN * na * nz
    obs_chunks = mapped_hbm.shape[2] // CHUNK
    chunks = obs_chunks + 1
    patches = nx * nz * nc
    near = nz * NEAR // 16
    hop = nz // 2 - near
    x, z, c = lax.axis_index("x"), lax.axis_index("z"), lax.axis_index("c")
    a = x * nc + c

    barrier = pltpu.get_barrier_semaphore()

    def signal_z(sem, step):
        pl.semaphore_signal(
            sem, inc=1, device_id={"z": lax.rem(z + nz + step, nz)}, device_id_type=MESH_ID
        )

    def greet_a(j, _):
        t = lax.rem(a + j, na)
        pl.semaphore_signal(
            barrier, inc=1, device_id={"x": t // nc, "c": lax.rem(t, nc)}, device_id_type=MESH_ID
        )
        return 0

    def raw_copies(k):
        if k < obs_chunks:
            src = lambda m: mapped_hbm.at[m, :, pl.ds(k * CHUNK, CHUNK)]
        else:
            src = lambda m: prior_hbm.at[m]
        return [
            pltpu.make_async_copy(src(m), raw.at[k, pl.ds(m * patches, patches)], raw_sem.at[k])
            for m in range(OWN)
        ]

    row_copies = [
        pltpu.make_async_copy(dep_hbm, dep_ref, row_sem.at[0]),
        pltpu.make_async_copy(prec_hbm, prec_ref, row_sem.at[1]),
    ]
    for step in range(near, 0, -1):
        signal_z(barrier, step)
        signal_z(barrier, -step)
    lax.fori_loop(1, na, greet_a, 0, unroll=True)
    for copy in raw_copies(0):
        copy.start()
    for k in range(1, chunks):
        for copy in raw_copies(k):
            copy.start()
    for copy in row_copies:
        copy.start()

    def natural(m, xi, zi, ci):
        return m * patches + xi * (nz * nc) + zi * nc + ci

    def of_natural(r):
        return r // patches, (r // (nz * nc)) % nx, (r // nc) % nz, r % nc

    def of_group(r):
        return r % OWN, r // (OWN * nz * nc), (r // OWN) % nz, (r // (OWN * nz)) % nc

    def of_ring(r):
        return r % OWN, (r // (OWN * nc)) % nx, r // (OWN * na), (r // OWN) % nc

    def group(m, xi, zi, ci):
        return ((xi * nc + ci) * nz + zi) * OWN + m

    def ring(m, xi, zi, ci):
        return ((zi * nx + xi) * nc + ci) * OWN + m

    columns = [
        (lax.rem(x + dx, nx), lax.rem(c + dc, nc))
        for dx in sorted(range(nx), key=lambda d: -min(d, nx - d))
        for dc in range(nc - 1, -1, -1)
    ]

    def z_copy(src, dst, send, recv, step):
        t = lax.rem(z + nz + step, nz)
        return pltpu.make_async_remote_copy(
            src_ref=src.at[t], dst_ref=dst.at[z], send_sem=send, recv_sem=recv,
            device_id={"z": t}, device_id_type=MESH_ID,
        )

    def all_a(src, dst, send, recv):
        for to_x, to_c in columns[:-1]:
            pltpu.make_async_remote_copy(
                src_ref=src.at[to_x * nc + to_c], dst_ref=dst.at[a], send_sem=send, recv_sem=recv,
                device_id={"x": to_x, "c": to_c}, device_id_type=MESH_ID,
            ).start()

    def ring_steps(most, least, *copy_args):
        def body(j, _):
            z_copy(*copy_args, most - j).start()
            z_copy(*copy_args, j - most).start()
            return 0

        lax.fori_loop(0, most - least + 1, body, 0, unroll=True)

    def ring_far(*copy_args):
        z_copy(*copy_args, nz // 2).start()
        if near + 1 < nz // 2:
            ring_steps(nz // 2 - 1, near + 1, *copy_args)

    def all_z(*copy_args):
        z_copy(*copy_args, nz // 2).start()
        ring_steps(nz // 2 - 1, 1, *copy_args)

    def arrived(name, ref, sem, n):
        part = ref.at[pl.ds(0, n)]
        with jax.named_scope(name):
            pltpu.make_async_copy(part, part, sem).wait()

    def by_group(perm, rows):
        return moved(perm[...], rows).reshape(na, OWN * nz, -1)

    def by_ring(perm, rows):
        return moved(perm[...], rows).reshape(nz, OWN * na, -1)

    def send_group(k):
        pltpu.make_async_copy(raw.at[k], raw.at[k], raw_sem.at[k]).wait()
        s1[k] = by_group(split_a, raw[k])
        all_a(s1.at[k], ar.at[k], a_send, a_recv.at[k])
        ar[k, a] = s1[k, a]

    def ring_args(k):
        return s2.at[k], zr.at[k], z_send, z_recv.at[k]

    def make_ring(k):
        pltpu.make_async_copy(raw.at[k], raw.at[k], raw_sem.at[k]).wait()
        s2[k] = by_ring(nat_z, raw[k])
        zr[k, z] = s2[k, z]

    nat_z[...] = one_hot(members, lambda r: natural(*of_ring(r)))
    make_ring(0)
    with jax.named_scope("greet"):
        pl.semaphore_wait(barrier, 2 * near + na - 1)
    signal_z(far, hop)
    signal_z(far, -hop)
    ring_steps(near, 1, *ring_args(0))
    for k in range(1, RING_FIRST):
        make_ring(k)
        ring_steps(near, 1, *ring_args(k))
    split_a[...] = one_hot(members, lambda r: natural(*of_group(r)))
    send_group(RING_FIRST)
    with jax.named_scope("far"):
        pl.semaphore_wait(far, 2)
    for k in range(RING_FIRST):
        ring_far(*ring_args(k))
    for k in range(RING_FIRST + 1, chunks):
        send_group(k)
    split_z[...] = one_hot(members, lambda r: group(*of_ring(r)))
    for k in range(RING_FIRST, chunks):
        arrived(f"a{k}", ar.at[k], a_recv.at[k], na - 1)
        rows = ar[k].reshape(members, CHUNK)
        if k < obs_chunks:
            s2[k] = by_ring(split_z, rows)
            all_z(*ring_args(k))
            zr[k, z] = s2[k, z]
        else:
            rows = moved(split_z[...], rows)
            for h in range(PIECES):
                s2p[h] = rows[:, h * HALF : (h + 1) * HALF].reshape(nz, OWN * na, HALF)
                all_z(s2p.at[h], zrp.at[h], p_send.at[h], p_recv.at[h])
                zrp[h, z] = s2p[h, z]
    back_z[...] = one_hot(members, lambda r: ring(*of_group(r)))
    z_nat[...] = one_hot(members, lambda r: ring(*of_natural(r)))

    for k in range(RING_FIRST):
        arrived(f"z{k}", zr.at[k], z_recv.at[k], nz - 1)
        s1[k] = by_group(back_z, zr[k].reshape(members, CHUNK))
        all_a(s1.at[k], ar.at[k], a_send, a_recv.at[k])
        ar[k, a] = s1[k, a]

    for copy in row_copies:
        copy.wait()
    lines = lines_ref[0]
    eye = (
        lax.broadcasted_iota(jnp.int32, (members, members), 0)
        == lax.broadcasted_iota(jnp.int32, (members, members), 1)
    )
    gram[...] = jnp.where(eye, f32(members - 1), f32(0.0))
    pull[...] = jnp.zeros_like(pull)
    for k in (*range(RING_FIRST, obs_chunks - 1), *range(RING_FIRST), obs_chunks - 1):
        if k < RING_FIRST:
            arrived(f"a{k}", ar.at[k], a_recv.at[k], na - 1)
            values = jnp.dot(
                split_z[...], ar[k].reshape(members, CHUNK), preferred_element_type=f32
            )
        else:
            arrived(f"z{k}", zr.at[k], z_recv.at[k], nz - 1)
            values = zr[k].reshape(members, CHUNK).astype(f32)
        with jax.named_scope("gram"):
            deviat = values - jnp.mean(values, axis=0, keepdims=True)
            row_ids = k * CHUNK + lax.broadcasted_iota(jnp.int32, (1, CHUNK), 1)
            cols = pl.ds(k * CHUNK, CHUNK)
            weights = jnp.where(row_ids < lines, prec_ref[:, cols], f32(0.0))
            weighted = deviat * weights
            gram[...] += product(halves(weighted), halves(deviat), 1, 1)
            pull[...] += jnp.sum(weighted * dep_ref[:, cols], axis=1, keepdims=True)

    with jax.named_scope("newton"):
        system = gram[...]
        scale = jnp.sqrt(
            jnp.sum(jnp.sum(system * system, axis=1, keepdims=True), axis=0, keepdims=True)
        )
        identity = jnp.where(eye, f32(1.5), f32(0.0))
        iterate = system / scale
        root = identity - 0.5 * iterate
        factor_halves = halves(root)
        root_halves = factor_halves
        iterate_halves = halves(product(halves(iterate), factor_halves))
        for sweep in range(1, ITERS):
            factor_halves = halves(identity - 0.5 * product(root_halves, iterate_halves))
            root = product(factor_halves, root_halves)
            if sweep < ITERS - 1:
                iterate_halves = halves(product(iterate_halves, factor_halves))
                root_halves = halves(root)

        inner = jnp.sum(root * pull[...], axis=0, keepdims=True)
        shift = jnp.sum(root * inner, axis=1, keepdims=True) / scale
        shift = jnp.sum(jnp.where(eye, shift, f32(0.0)), axis=0, keepdims=True)
        transform = (math.sqrt(members - 1) / jnp.sqrt(scale)) * root + shift
        kept = 1.0 - jnp.sum(transform, axis=1, keepdims=True)
        transform = halves(transform + kept / members)

    def result(h):
        arrived(f"p{h}", zrp.at[h], p_recv.at[h], nz - 1)
        quantities = zrp[h].reshape(members, HALF)
        return (
            jnp.dot(transform[0], quantities, preferred_element_type=f32)
            + jnp.dot(transform[1], quantities, preferred_element_type=f32)
        ).astype(bf16)

    for h in range(PIECES):
        s5[h] = result(h).reshape(s5.shape[1:])

        def straight(step):
            t = lax.rem(z + nz + step, nz)
            own = isinstance(step, int) and step == 0
            for to_x, to_c in columns[:-1] if own else columns:
                pltpu.make_async_remote_copy(
                    src_ref=s5.at[h, (t * nx + to_x) * nc + to_c], dst_ref=db.at[h, z * na + a],
                    send_sem=db_send.at[h], recv_sem=db_recv.at[h],
                    device_id={"x": to_x, "z": t, "c": to_c}, device_id_type=MESH_ID,
                ).start()

        def straight_both(j, _):
            straight(nz // 2 - 1 - j)
            straight(j - nz // 2 + 1)
            return 0

        straight(nz // 2)
        lax.fori_loop(0, nz // 2 - 1, straight_both, 0, unroll=True)
        straight(0)
        db[h, z * na + a] = s5[h, z * na + a]
    for h in range(PIECES):
        arrived(f"straight{h}", db.at[h], db_recv.at[h], na * nz - 1)
        rows = moved(z_nat[...], db[h].reshape(members, HALF))
        out_ref[:, :, h * HALF : (h + 1) * HALF] = rows.reshape(OWN, patches, HALF)
    for h in range(PIECES):
        arrived("sent", s5.at[h], db_send.at[h], na * nz - 1)

    for part, sem in (
        (s1.at[:, pl.ds(0, na - 1)], a_send), (s2.at[:, pl.ds(0, nz - 1)], z_send)
    ):
        pltpu.make_async_copy(part, part, sem).wait()
    for half in range(PIECES):
        arrived("sent", s2p.at[half], p_send.at[half], nz - 1)


def solution(mesh):
    nx, nz, nc = 4, 16, 2
    split = Mesh(mesh.devices.reshape(nx, nz, nc, mesh.shape["grp"]), ("x", "z", "c", "grp"))
    na = nx * nc
    members = OWN * na * nz

    def local(prior_members, mapped_prior, departure, precision_factor, measured_lines):
        chunks = mapped_prior.shape[2] // CHUNK + 1
        perm = pltpu.VMEM((members, members), bf16)
        by_a = (na, OWN * nz)
        by_z = (nz, OWN * na)
        dma = pltpu.SemaphoreType.DMA
        return pl.pallas_call(
            functools.partial(kernel, nx, nz, nc),
            out_shape=jax.ShapeDtypeStruct(prior_members.shape, bf16),
            in_specs=[
                pl.BlockSpec(memory_space=pltpu.HBM),
                pl.BlockSpec(memory_space=pltpu.HBM),
                pl.BlockSpec(memory_space=pltpu.HBM),
                pl.BlockSpec(memory_space=pltpu.HBM),
                pl.BlockSpec(memory_space=pltpu.SMEM),
            ],
            out_specs=pl.BlockSpec(memory_space=pltpu.VMEM),
            scratch_shapes=[
                pltpu.VMEM((chunks, members, CHUNK), bf16),
                pltpu.VMEM(departure.shape, f32),
                pltpu.VMEM(precision_factor.shape, f32),
                perm, perm, perm, perm, perm,
                pltpu.VMEM((chunks, *by_a, CHUNK), bf16),
                pltpu.VMEM((chunks, *by_a, CHUNK), bf16),
                pltpu.VMEM((chunks - 1, *by_z, CHUNK), bf16),
                pltpu.VMEM((chunks - 1, *by_z, CHUNK), bf16),
                pltpu.VMEM((PIECES, *by_z, HALF), bf16),
                pltpu.VMEM((PIECES, *by_z, HALF), bf16),
                pltpu.VMEM((PIECES, na * nz, OWN, HALF), bf16),
                pltpu.VMEM((PIECES, na * nz, OWN, HALF), bf16),
                pltpu.VMEM((members, members), f32),
                pltpu.VMEM((members, 1), f32),
                dma((chunks,)),
                dma((2,)),
                pltpu.SemaphoreType.REGULAR,
                dma, dma((chunks,)),
                dma, dma((chunks - 1,)),
                dma((PIECES,)), dma((PIECES,)),
                dma((PIECES,)), dma((PIECES,)),
            ],
            compiler_params=pltpu.CompilerParams(
                collective_id=0, has_side_effects=True, vmem_limit_bytes=48 << 20
            ),
        )(
            *(
                pltpu.with_memory_space_constraint(array, pltpu.HBM)
                for array in (
                    prior_members, mapped_prior, departure, precision_factor,
                )
            ),
            measured_lines,
        )

    return jax.shard_map(
        local,
        mesh=split,
        in_specs=(
            P(MEM, "grp", None),
            P(MEM, "grp", None),
            P(GRP_MEM, None),
            P(GRP_MEM, None),
            P(GRP_MEM),
        ),
        out_specs=P(MEM, "grp", None),
        check_vma=False,
    )
```
